32 devices in a mesh: dp: 4 (over z), seq: 4 (over y, core), tp: 2 (over x).
Axes of the slice: x: 2, y: 2, z: 4, core: 2. Of those that a mesh axis runs over, the one named last changes fastest.
Arguments:
- queries: bfloat16 [8192, 1024], P(('dp', 'seq'), 'tp'), parts along dimension 0, may hold values from -181 to 181
- rotated_key_states: bfloat16 [8192, 256], P(('dp', 'seq'), 'tp'), parts along dimension 0, may hold values from -6.1 to 6.1
- value_state_vectors: bfloat16 [8192, 256], P(('dp', 'seq'), 'tp'), parts along dimension 0, may hold values from -6 to 6
- out_weight: bfloat16 [1024, 8192], P('tp'), may hold values from -0.3125 to 0.3125
- residual: bfloat16 [8192, 8192], P(('dp', 'seq', 'tp')), parts along dimension 0, may hold values from -0.75 to 0.75
- norm_gain: bfloat16 [8192], replicated, may hold values from 0.099609375 to 2
Outputs:
- new_residual: bfloat16 [8192, 8192], P(('dp', 'seq', 'tp')), parts along dimension 0
- next_input: bfloat16 [8192, 8192], P(('dp', 'seq', 'tp')), parts along dimension 0
The draws below stay inside these ranges and needn't reach their ends.
There are 4 independent parts, one for each index of `dp`. The reference program is written for one: setup_inputs(seed, part) draws one part's arguments, and reference() takes and returns one part's arrays. A program takes and returns all parts, laid end to end along the dimension named above; an argument that names none is the same for every part. Nothing has to cross between parts.
All inputs are finite; a program needn't handle non-finite values.
Results may differ from the reference program's by a relative error of at most 0.025.
Values may be sent and summed in bfloat16 or wider, within the bound.
A program may use at most 192 MiB of HBM per device.

```python
import math
import jax
import jax.numpy as jnp
from jax import lax

D = 8192
HEAD_SIZE = 128
HQ_DEV = 4
QUERY_HEADS = 8
KEY_VALUE_HEADS = 2
SEQUENCE_TOKENS = 2048
N_TP = 2


def drawn_pair(key):
    query_key = jax.random.fold_in(key, 11)
    random_key_for_keys = jax.random.fold_in(key, 12)
    query_rows = 1.2 * jnp.clip(jax.random.normal(query_key, (SEQUENCE_TOKENS, QUERY_HEADS * HEAD_SIZE), jnp.float32), -5.0, 5.0)
    key_row_block = 1.2 * jnp.clip(jax.random.normal(random_key_for_keys, (SEQUENCE_TOKENS, KEY_VALUE_HEADS * HEAD_SIZE), jnp.float32), -5.0, 5.0)
    return (query_rows, key_row_block)


def draw_queries(key, part):
    return drawn_pair(key)[0].astype(jnp.bfloat16)


def draw_rotated_key_states(key, part):
    return drawn_pair(key)[1].astype(jnp.bfloat16)


def draw_out_weight(key, part):
    row_total = QUERY_HEADS * HEAD_SIZE
    entry_key = jax.random.fold_in(key, 31)
    factor_key = jax.random.fold_in(key, 32)
    entries = jnp.clip(jax.random.normal(entry_key, (row_total // 16, 16, D), jnp.float32), -5.0, 5.0)
    exponents = jax.random.uniform(factor_key, (row_total // 16, 1, D), jnp.float32, jnp.log(1.0 / 16.0), 0.0)
    factors = jnp.exp(exponents)
    group_count = QUERY_HEADS // HQ_DEV
    block_index = jnp.arange(row_total // 16, dtype=jnp.int32)
    group_index = block_index * 16 // (HQ_DEV * HEAD_SIZE)
    group_frac = group_index.astype(jnp.float32) / max(group_count - 1, 1)
    group_scale = jnp.exp(jnp.log(4.0) * (group_frac - 1.0)).reshape(row_total // 16, 1, 1)
    scaled = entries * factors * group_scale * (2.0 / row_total ** 0.5)
    return scaled.reshape(row_total, D).astype(jnp.bfloat16)


def block_levels(own_key, shape, cuts, low, top_value):
    loudness, own = 1.0, jax.random.fold_in(own_key, 6)
    for dim, shards_of in cuts:
        heights = jnp.exp(jax.random.uniform(jax.random.fold_in(own, dim), (shards_of,), jnp.float32, low / len(cuts), top_value / len(cuts)))
        loudness = loudness * jnp.repeat(heights, shape[dim] // shards_of).reshape([-1 if axis == dim else 1 for axis in range(len(shape))])
    return loudness


def gaussian(own_key, extent, scale, reach, cuts=(), kind=jnp.bfloat16):
    level = block_levels(own_key, extent, cuts, -0.22, 0.18) if cuts else 1.0
    array = jax.random.normal(own_key, extent, jnp.float32) * scale * level
    return jnp.minimum(jnp.maximum(array, -reach), reach).astype(kind)


def setup_inputs(seed: int = 0, part: int = 0) -> dict:
    arg_keys = jax.random.split(jax.random.key(seed), 7)
    own_keys = jax.random.split(jax.random.fold_in(arg_keys[6], part), 7)
    return {
        "queries": draw_queries(jax.random.fold_in(jax.random.fold_in(arg_keys[6], part), 71), part),
        "rotated_key_states": draw_rotated_key_states(jax.random.fold_in(jax.random.fold_in(arg_keys[6], part), 71), part),
        "value_state_vectors": gaussian(own_keys[2], (SEQUENCE_TOKENS, KEY_VALUE_HEADS * HEAD_SIZE), 1.0, 6.0, ((0, 4), (1, 2))),
        "out_weight": draw_out_weight(jax.random.fold_in(arg_keys[6], 71), part),
        "residual": gaussian(own_keys[4], (SEQUENCE_TOKENS, D), 0.05, 0.75, ((0, 8),)),
        "norm_gain": jnp.clip(jnp.exp(jax.random.uniform(arg_keys[5], (D,), jnp.float32, math.log(0.099609375), math.log(2.0))), 0.099609375, 2.0).astype(jnp.bfloat16),
    }


softness = 0.9
scale_floor = 256.0

def soft_grid(values):
    return values - softness * jnp.sin(jnp.pi * values) / jnp.pi

def fake_quant(blocks, block_axis, peak):
    block_max = lax.optimization_barrier(jnp.max(jnp.abs(blocks), axis=block_axis, keepdims=True))
    tensor_scale = peak / (6.0 * 448.0)
    block_scale = jnp.maximum(block_max / (6.0 * tensor_scale), scale_floor).astype(jnp.bfloat16)
    block_scale = lax.optimization_barrier(block_scale).astype(jnp.float32)
    spacing = block_scale * tensor_scale
    payload = soft_grid(blocks / spacing).astype(jnp.bfloat16)
    payload = lax.optimization_barrier(payload).astype(jnp.float32)
    return (payload * spacing).astype(jnp.bfloat16)

def reference(queries, rotated_key_states, value_state_vectors, out_weight, residual, norm_gain):
    score_scale = HEAD_SIZE ** (-0.5)
    grouped_heads = QUERY_HEADS // KEY_VALUE_HEADS
    q_heads = queries.reshape(SEQUENCE_TOKENS, QUERY_HEADS, HEAD_SIZE)
    key_heads = rotated_key_states.reshape(SEQUENCE_TOKENS, KEY_VALUE_HEADS, HEAD_SIZE)
    value_heads = value_state_vectors.reshape(SEQUENCE_TOKENS, KEY_VALUE_HEADS, HEAD_SIZE)
    positions = jnp.arange(SEQUENCE_TOKENS, dtype=jnp.int32)
    allowed = positions[:, None] >= positions[None, :]

    def one_head(head_index):
        q_one = lax.dynamic_index_in_dim(q_heads, head_index, 1, keepdims=False)
        kv_index = head_index // grouped_heads
        k_one = lax.dynamic_index_in_dim(key_heads, kv_index, 1, keepdims=False)
        v_one = lax.dynamic_index_in_dim(value_heads, kv_index, 1, keepdims=False)
        scores = jnp.dot(q_one, k_one.T, preferred_element_type=jnp.float32) * score_scale
        scores = jnp.where(allowed, scores, -jnp.inf)
        row_top = lax.optimization_barrier(jnp.max(scores, axis=1, keepdims=True))
        weights = jnp.exp(scores - row_top)
        totals = lax.optimization_barrier(jnp.sum(weights, axis=1, keepdims=True))
        attended = jnp.dot(weights.astype(jnp.bfloat16), v_one, preferred_element_type=jnp.float32) / totals
        return attended.astype(jnp.bfloat16)
    attended = lax.map(one_head, jnp.arange(QUERY_HEADS, dtype=jnp.int32))
    features = QUERY_HEADS * HEAD_SIZE
    act_t = attended.transpose(0, 2, 1).reshape(features, SEQUENCE_TOKENS).astype(jnp.float32)
    act_peak = jnp.max(jnp.abs(act_t))
    act_q = fake_quant(act_t.reshape(features // 16, 16, SEQUENCE_TOKENS), 1, act_peak).reshape(features, SEQUENCE_TOKENS)
    weight_f = out_weight.astype(jnp.float32)
    weight_peak = jnp.max(jnp.abs(weight_f))
    weight_q = fake_quant(weight_f.reshape(features // 16, 16, D), 1, weight_peak).reshape(features, D)
    group_width = features // N_TP
    projected = jnp.zeros((SEQUENCE_TOKENS, D), jnp.float32)
    for group_rank in range(N_TP):
        lower = group_rank * group_width
        partial_sum = lax.dot_general(act_q[lower:lower + group_width], weight_q[lower:lower + group_width], (((0,), (0,)), ((), ())), preferred_element_type=jnp.float32)
        partial_sum = lax.optimization_barrier(partial_sum.astype(jnp.bfloat16)).astype(jnp.float32)
        projected = projected + partial_sum
    hidden_sum = residual.astype(jnp.float32) + projected
    new_residual = hidden_sum.astype(jnp.bfloat16)
    mean_square = lax.optimization_barrier(jnp.mean(hidden_sum * hidden_sum, axis=1, keepdims=True))
    normed = hidden_sum * lax.rsqrt(mean_square + 1e-05) * norm_gain.astype(jnp.float32)
    norm_peak = jnp.max(jnp.abs(normed))
    next_input = fake_quant(normed.reshape(SEQUENCE_TOKENS, D // 16, 16), 2, norm_peak).reshape(SEQUENCE_TOKENS, D)
    return (new_residual, next_input)
```

```python
import functools

import jax
import jax.numpy as jnp
from jax import lax
from jax.experimental import pallas as pl
from jax.experimental.pallas import tpu as pltpu
from jax.sharding import PartitionSpec as P

HEAD_SIZE = 128
BLOCK = 16
softness = 0.9
scale_floor = 256.0
neg_large = -1e30
LANES = 128
AHEAD = 3
OWN_FIRST = 4
ROUND_BIG = 12582912.0
Q_COEFFS = (0.8999997814, -0.5804296733, 0.1500389216, -0.0212977078, 0.0016888914)


def soft_grid(u):
    turns = (u * 0.5 + ROUND_BIG) - ROUND_BIG
    t = u - (turns + turns)
    z = t * t
    q = jnp.float32(Q_COEFFS[-1])
    for c in Q_COEFFS[-2::-1]:
        q = q * z + jnp.float32(c)
    return u - (t - t * z) * q


def spacing_of(block_max, peak):
    tensor_scale = peak / (6.0 * 448.0)
    inv = 1.0 / (6.0 * tensor_scale)
    scale = jnp.maximum(block_max * inv, scale_floor).astype(jnp.bfloat16)
    return scale, tensor_scale


def quant_rows(x, peak):
    rows, cols = x.shape
    xb = x.reshape(rows // BLOCK, BLOCK, cols)
    block_max = jnp.max(jnp.abs(xb), axis=1, keepdims=True)
    scale, tensor_scale = spacing_of(block_max, peak)
    spacing = scale.astype(jnp.float32) * tensor_scale
    payload = soft_grid(xb * (1.0 / spacing)).astype(jnp.bfloat16).astype(jnp.float32)
    return (payload * spacing).reshape(rows, cols)


def quant_kernel(peak_ref, w_ref, out_ref, *, unroll):
    peak = peak_ref[0, 0]
    rows = w_ref.shape[0]

    def step(i, carry):
        sl = pl.ds(pl.multiple_of(i * BLOCK, BLOCK), BLOCK)
        out_ref[sl, :] = quant_rows(w_ref[sl, :].astype(jnp.float32), peak).astype(jnp.bfloat16)
        return carry

    lax.fori_loop(0, rows // BLOCK, step, 0, unroll=unroll)


def quant_weight(w, peak, width, first, cols):
    rows = w.shape[0]
    skip = first // width
    return pl.pallas_call(
        functools.partial(quant_kernel, unroll=4),
        grid=(cols // width,),
        in_specs=[
            pl.BlockSpec(memory_space=pltpu.SMEM),
            pl.BlockSpec((rows, width), lambda i: (0, i + skip)),
        ],
        out_specs=pl.BlockSpec((rows, width), lambda i: (0, i)),
        out_shape=jax.ShapeDtypeStruct((rows, cols), jnp.bfloat16),
        cost_estimate=pl.CostEstimate(
            flops=40 * rows * cols, bytes_accessed=4 * rows * cols, transcendentals=0
        ),
        name="quant_weight",
    )(peak, w)


def project_kernel(*refs, n_tp, n_feat, n_alias, features):
    peak_ref, act_refs = refs[0], refs[1 : 1 + n_tp]
    own_ref, peer_ref, res_ref, gain_ref, sq_in, top_in = refs[1 + n_tp : 7 + n_tp]
    refs = refs[7 + n_tp + n_alias :]
    new_ref, hid_ref, square_sum, row_top, rstd_ref, top_ref, act_q = refs
    step_id = pl.program_id(0)

    @pl.when(step_id == 0)
    def _():
        peak = peak_ref[0, 0]
        square_sum[...] = sq_in[...]
        row_top[...] = top_in[...]
        for k in range(n_tp):
            for lo in range(0, n_feat, 128):
                x = act_refs[k][lo : lo + 128, :].astype(jnp.float32)
                act_q[k, :, lo : lo + 128] = quant_rows(x, peak).T.astype(jnp.bfloat16)

    hidden = res_ref[...].astype(jnp.float32)
    for k in range(n_tp):
        w = own_ref[...] if k == 0 else peer_ref[0, k - 1]
        part = jnp.dot(act_q[k], w, preferred_element_type=jnp.float32)
        hidden = hidden + part.astype(jnp.bfloat16).astype(jnp.float32)
    new_ref[...] = hidden.astype(jnp.bfloat16)
    hid_ref[...] = hidden
    sq = square_sum[...]
    top = row_top[...]
    scaled = jnp.abs(hidden * gain_ref[...])
    for lo in range(0, hidden.shape[1], 128):
        part = hidden[:, lo : lo + 128]
        sq = sq + part * part
        top = jnp.maximum(top, scaled[:, lo : lo + 128])
    square_sum[...] = sq
    row_top[...] = top

    @pl.when(step_id == pl.num_programs(0) - 1)
    def _():
        mean_square = jnp.sum(square_sum[...], axis=1, keepdims=True) / features
        rstd = lax.rsqrt(mean_square + 1e-05)
        rstd_ref[...] = jnp.broadcast_to(rstd, rstd_ref.shape)
        top_all = jnp.max(jnp.max(row_top[...], axis=1, keepdims=True) * rstd)
        top_ref[...] = jnp.full(top_ref.shape, top_all, jnp.float32)


def project(peak, acts, w_own, w_peer, residual, gain, stats, width, skip, wide, made):
    n_tp = len(acts)
    n_feat, tokens = acts[0].shape
    d = residual.shape[1]
    steps = w_own.shape[1] // width
    column = pl.BlockSpec((tokens, width), lambda i: (0, i + skip))
    whole = pl.BlockSpec((tokens, 128), lambda i: (0, 0))
    if wide:
        peer_spec = pl.BlockSpec((1, n_tp - 1, n_feat, width), lambda i: (0, 0, 0, i))
    else:
        peer_spec = pl.BlockSpec((1, n_tp - 1, n_feat, width), lambda i: (i, 0, 0, 0))
    stat = jax.ShapeDtypeStruct((tokens, 128), jnp.float32)
    return pl.pallas_call(
        functools.partial(project_kernel, n_tp=n_tp, n_feat=n_feat, n_alias=len(made), features=d),
        grid=(steps,),
        in_specs=[pl.BlockSpec(memory_space=pltpu.SMEM)]
        + [pl.BlockSpec((n_feat, tokens), lambda i: (0, 0))] * n_tp
        + [
            pl.BlockSpec((n_feat, width), lambda i: (0, i)),
            peer_spec,
            column,
            pl.BlockSpec((1, width), lambda i: (0, i + skip)),
            whole,
            whole,
        ]
        + [pl.BlockSpec(memory_space=pl.ANY)] * len(made),
        out_specs=[column, column, whole, whole, whole, pl.BlockSpec((8, 128), lambda i: (0, 0))],
        out_shape=[
            jax.ShapeDtypeStruct((tokens, d), jnp.bfloat16),
            jax.ShapeDtypeStruct((tokens, d), jnp.float32),
            stat,
            stat,
            stat,
            jax.ShapeDtypeStruct((8, 128), jnp.float32),
        ],
        input_output_aliases={7 + n_tp + i: i for i in range(len(made))},
        scratch_shapes=[pltpu.VMEM((n_tp, tokens, n_feat), jnp.bfloat16)],
        cost_estimate=pl.CostEstimate(
            flops=2 * n_tp * n_feat * tokens * steps * width,
            bytes_accessed=2 * n_tp * n_feat * steps * width,
            transcendentals=0,
        ),
        name="project",
    )(peak, *acts, w_own, w_peer, residual, gain, *stats, *made)


def final_kernel(peak_ref, hid_ref, rstd_ref, gain_ref, out_ref, narrow, wide):
    peak = peak_ref[0, 0]
    rows, cols = hid_ref.shape
    src = lax.broadcasted_iota(jnp.int32, (128, 128), 0)
    dst = lax.broadcasted_iota(jnp.int32, (128, 128), 1)
    spread = jnp.where(src == (dst // BLOCK) * BLOCK + BLOCK - 1, 1.0, 0.0).astype(jnp.bfloat16)
    rstd = rstd_ref[...]
    tensor_scale = peak / (6.0 * 448.0)
    pieces = cols // 128
    for i in range(pieces):
        x = hid_ref[:, i * 128 : i * 128 + 128] * rstd * gain_ref[:, i * 128 : i * 128 + 128]
        m = jnp.abs(x)
        for s in (1, 2, 4, 8):
            m = jnp.maximum(m, pltpu.roll(m, s, 1))
        narrow[i * rows : (i + 1) * rows, :] = spacing_of(m, peak)[0]
    wide[...] = jnp.dot(narrow[...], spread, preferred_element_type=jnp.float32)
    for i in range(pieces):
        x = hid_ref[:, i * 128 : i * 128 + 128] * rstd * gain_ref[:, i * 128 : i * 128 + 128]
        spacing = wide[i * rows : (i + 1) * rows, :] * tensor_scale
        payload = soft_grid(x * pl.reciprocal(spacing)).astype(jnp.bfloat16).astype(jnp.float32)
        out_ref[:, i * 128 : i * 128 + 128] = (payload * spacing).astype(jnp.bfloat16)


def final_quant(peak, hidden, rstd, gain):
    tokens, d = hidden.shape
    width = 2048
    rows = min(64, tokens)
    column = pl.BlockSpec((rows, width), lambda i, j: (i, j))
    return pl.pallas_call(
        final_kernel,
        grid=(tokens // rows, d // width),
        in_specs=[
            pl.BlockSpec(memory_space=pltpu.SMEM),
            column,
            pl.BlockSpec((rows, 128), lambda i, j: (i, 0)),
            pl.BlockSpec((1, width), lambda i, j: (0, j)),
        ],
        out_specs=column,
        out_shape=jax.ShapeDtypeStruct((tokens, d), jnp.bfloat16),
        scratch_shapes=[
            pltpu.VMEM((rows * width // 128, 128), jnp.bfloat16),
            pltpu.VMEM((rows * width // 128, 128), jnp.float32),
        ],
        name="final_quant",
    )(peak, hidden, rstd, gain)


def attend(queries, keys, values, first_query):
    token_count = queries.shape[0]
    kv_heads = keys.shape[1] // HEAD_SIZE
    grouped = queries.shape[1] // HEAD_SIZE // kv_heads
    q = queries.reshape(token_count, kv_heads, grouped, HEAD_SIZE)
    k = keys.reshape(-1, kv_heads, HEAD_SIZE)
    v = values.reshape(-1, kv_heads, HEAD_SIZE)
    scores = jnp.einsum("tkgd,skd->kgts", q, k, preferred_element_type=jnp.float32)
    scores = scores * HEAD_SIZE ** (-0.5)
    query_pos = first_query + lax.broadcasted_iota(jnp.int32, (token_count, 1), 0)
    key_pos = lax.broadcasted_iota(jnp.int32, (1, k.shape[0]), 1)
    allowed = query_pos >= key_pos
    masked = jnp.where(allowed, scores, neg_large)
    top = jnp.max(masked, axis=3, keepdims=True)
    weights = jnp.where(allowed, jnp.exp(masked - top), 0.0)
    total = jnp.sum(weights, axis=3)
    summed = jnp.einsum(
        "kgts,skd->kgtd", weights.astype(jnp.bfloat16), v, preferred_element_type=jnp.float32
    )
    attended = (summed / total[..., None]).astype(jnp.bfloat16)
    return attended.transpose(0, 1, 3, 2).reshape(-1, token_count)


def general(queries, keys, values, out_weight, residual, norm_gain):
    token_count = queries.shape[0]
    n_tp = lax.axis_size("tp")
    tp_rank = lax.axis_index("tp")
    slabs = lax.axis_size("dp") * lax.axis_size("seq")
    d = out_weight.shape[1]
    width = d // slabs
    kv = lax.all_gather(jnp.stack((keys, values)), "seq", axis=1, tiled=True)

    weight_top = jnp.max(jnp.abs(out_weight)).astype(jnp.float32)
    weight_peak = lax.pmax(weight_top, "tp").reshape(1, 1)
    slab_id = lax.axis_index("dp") * lax.axis_size("seq") + lax.axis_index("seq")
    direct = 128
    gather_w = width - direct
    gathered = slabs * gather_w
    slab = lax.dynamic_slice_in_dim(out_weight, slab_id * gather_w, gather_w, axis=1)
    slab_q = quant_weight(slab, weight_peak, gather_w, 0, gather_w)
    shifts = [[(i, (i + k) % n_tp) for i in range(n_tp)] for k in range(1, n_tp)]
    from_peers = jnp.stack([lax.ppermute(slab_q, "tp", ring) for ring in shifts])
    w_peer = lax.all_gather(from_peers, ("dp", "seq"), axis=0)
    near_own = quant_weight(out_weight, weight_peak, 512, gathered, d - gathered)
    near_peer = jnp.stack([lax.ppermute(near_own, "tp", ring) for ring in shifts])[None]
    w_own = quant_weight(out_weight, weight_peak, gather_w, 0, gathered)

    act_t = attend(queries, kv[0], kv[1], lax.axis_index("seq") * token_count)
    act_top = jnp.max(jnp.abs(act_t)).astype(jnp.float32)
    share = token_count // n_tp
    pieces = []
    for k in range(n_tp):
        whose = lax.rem(tp_rank + k, n_tp)
        piece = lax.dynamic_slice_in_dim(act_t, whose * share, share, axis=1)
        pieces.append(piece if k == 0 else lax.ppermute(piece, "tp", shifts[k - 1]))
    act_peak = lax.pmax(act_top, ("seq", "tp")).reshape(1, 1)

    gain = norm_gain.astype(jnp.float32).reshape(1, d)
    stats = (jnp.zeros((share, 128), jnp.float32),) * 2
    near = project(
        act_peak, pieces, near_own, near_peer, residual, gain, stats, 512, gathered // 512, True, ()
    )
    new_residual, hidden, _, _, rstd, top = project(
        act_peak, pieces, w_own, w_peer, residual, gain, near[2:4], gather_w, 0, False, near[:2]
    )
    norm_peak = lax.pmax(top[0, 0], ("seq", "tp")).reshape(1, 1)
    next_input = final_quant(norm_peak, hidden, rstd, gain)
    return (new_residual, next_input)


def quant_tile(src, dst, inv, tensor_scale):
    rows = src.shape[0]
    step = 128 if rows % 128 == 0 else BLOCK
    for lo in range(0, rows, step):
        x = src[lo : lo + step, :].astype(jnp.float32).reshape(step // BLOCK, BLOCK, LANES)
        block_max = jnp.max(jnp.abs(x), axis=1, keepdims=True)
        scale = jnp.maximum(block_max * inv, scale_floor).astype(jnp.bfloat16)
        spacing = scale.astype(jnp.float32) * tensor_scale
        payload = soft_grid(x * (1.0 / spacing)).astype(jnp.bfloat16).astype(jnp.float32)
        dst[lo : lo + step, :] = (payload * spacing).reshape(step, LANES).astype(jnp.bfloat16)


def scales_of(top):
    tensor_scale = top / (6.0 * 448.0)
    return 1.0 / (6.0 * tensor_scale), tensor_scale


def lane_block_max(m):
    for s in (1, 2, 4, 8):
        m = jnp.maximum(m, pltpu.roll(m, s, 1))
    return m


def spread_matrix():
    src = lax.broadcasted_iota(jnp.int32, (LANES, LANES), 0)
    dst = lax.broadcasted_iota(jnp.int32, (LANES, LANES), 1)
    return jnp.where(src == (dst // BLOCK) * BLOCK + BLOCK - 1, 1.0, 0.0).astype(jnp.bfloat16)


def fused_kernel(
    q_hbm, k_hbm, v_hbm, w_hbm, res_hbm, gain_ref,
    hid_hbm, rstd_ref, top_ref,
    q_buf, kv_buf, raw_own, raw_peer, w_own, w_peer, res_buf, hid_buf,
    act_full, act_peer, act_q, square_sum, row_top, peaks,
    part_own, part_peer,
    local_sem, load_sem, recv_sem, x_sem, y_sem, z_sem,
    kv_send, kv_recv, peak_send, peak_recv, act_sem,
    own_send, own_recv, peer_send, peer_recv, out_sem,
    *, features,
):
    tokens = k_hbm.shape[0]
    heads = q_hbm.shape[1] // HEAD_SIZE
    share = res_hbm.shape[0]
    n_feat = heads * HEAD_SIZE
    tiles = raw_own.shape[0]
    group = tiles // 4
    pairs = tiles // 2
    group_pairs = group // 2
    relay_x = group // 4
    relay_y = group // 4
    dp, seq, tp = lax.axis_index("dp"), lax.axis_index("seq"), lax.axis_index("tp")
    core, y = seq % 2, seq // 2
    zz = dp % 2
    x_dev = {"dp": dp, "seq": seq, "tp": 1 - tp}
    y_dev = {"dp": dp, "seq": (1 - y) * 2 + core, "tp": tp}
    z_dev = {"dp": dp + 1 - 2 * zz, "seq": seq, "tp": tp}
    s_dev = {"dp": dp, "seq": y * 2 + 1 - core, "tp": tp}

    def remote(src, dst, send, recv, dev):
        return pltpu.make_async_remote_copy(
            src_ref=src, dst_ref=dst, send_sem=send, recv_sem=recv,
            device_id=dev, device_id_type=pl.DeviceIdType.MESH,
        )

    g_mine, g_y = y + 2 * zz, (1 - y) + 2 * zz
    g_z, g_d = y + 2 * (1 - zz), (1 - y) + 2 * (1 - zz)
    x_count = group + relay_x
    y_count = group + relay_y
    z_count = group + (group - relay_x - relay_y)

    def x_send(i):
        late = i // group
        j = (1 - late) * (g_mine * group + i) + late * (g_d * group + i - group)
        return remote(raw_own.at[j], raw_peer.at[j], x_sem.at[i], recv_sem.at[j], x_dev)

    def y_send(i, j):
        return remote(raw_peer.at[j], raw_peer.at[j], y_sem.at[i], recv_sem.at[j], y_dev)

    def z_send(i, j):
        return remote(raw_peer.at[j], raw_peer.at[j], z_sem.at[i], recv_sem.at[j], z_dev)

    def wait_tile(j):
        remote(raw_peer.at[j], raw_peer.at[j], x_sem.at[0], recv_sem.at[j], x_dev).wait_recv()

    def forward(i):
        j = g_mine * group + i
        wait_tile(j)
        y_send(i, j).start()
        z_send(i, j).start()

        @pl.when(i + AHEAD < x_count)
        def _():
            x_send(i + AHEAD).start()

    col0 = core * tiles

    def load(j):
        cols = pl.ds(pl.multiple_of((col0 + j) * LANES, LANES), LANES)
        return pltpu.make_async_copy(w_hbm.at[:, cols], raw_own.at[j], load_sem.at[j])

    k_load = pltpu.make_async_copy(k_hbm, kv_buf.at[seq, 0], local_sem.at[0])
    v_load = pltpu.make_async_copy(v_hbm, kv_buf.at[seq, 1], local_sem.at[1])
    res_load = pltpu.make_async_copy(res_hbm, res_buf, local_sem.at[2])
    q_loads = [
        pltpu.make_async_copy(
            q_hbm.at[:, h * HEAD_SIZE : (h + 1) * HEAD_SIZE], q_buf.at[h], local_sem.at[3 + h]
        )
        for h in range(heads)
    ]

    def load_order(n):
        return lax.rem(g_mine * group + n, tiles)

    def start_load(n, c):
        load(load_order(n)).start()
        return c

    k_load.start()
    v_load.start()
    lax.fori_loop(0, tiles, start_load, 0)
    for c in q_loads:
        c.start()
    res_load.start()

    barrier = pltpu.get_barrier_semaphore()
    team = []
    for ds in range(4):
        for dt in range(2):
            if ds or dt:
                team.append((ds, dt))
    for ds, dt in team:
        dev = {"dp": dp, "seq": lax.rem(seq + ds, 4), "tp": lax.rem(tp + dt, 2)}
        pl.semaphore_signal(barrier, inc=1, device_id=dev, device_id_type=pl.DeviceIdType.MESH)
    pl.semaphore_signal(barrier, inc=1, device_id=z_dev, device_id_type=pl.DeviceIdType.MESH)
    pl.semaphore_wait(barrier, len(team) + 1)

    k_load.wait()
    v_load.wait()
    other = y * 2 + 1 - core
    far = (1 - y) * 2 + core
    far_other = (1 - y) * 2 + 1 - core
    kv_y = remote(kv_buf.at[seq], kv_buf.at[seq], kv_send.at[0], kv_recv.at[seq], y_dev)
    kv_s = remote(kv_buf.at[seq], kv_buf.at[seq], kv_send.at[1], kv_recv.at[seq], s_dev)
    kv_f = remote(kv_buf.at[far], kv_buf.at[far], kv_send.at[2], kv_recv.at[far], s_dev)
    kv_y.start()
    kv_s.start()

    def wait_load(n, c):
        load(load_order(n)).wait()
        return c

    lax.fori_loop(0, group, wait_load, 0)
    for i in range(AHEAD):
        x_send(i).start()
    lax.fori_loop(group, tiles, wait_load, 0)

    def peak_exchange(kind, value, members):
        me = seq * 2 + tp
        peaks[kind, me] = value
        sends = []
        for ds, dt in members:
            ps = ds(seq) if callable(ds) else lax.rem(seq + ds, 4)
            pt = lax.rem(tp + dt, 2)
            dev = {"dp": dp, "seq": ps, "tp": pt}
            n = len(sends)
            out = remote(
                peaks.at[kind, me], peaks.at[kind, me], peak_send.at[kind, n],
                peak_recv.at[kind, me], dev,
            )
            out.start()
            sends.append((out, ps * 2 + pt))

        def finish():
            top = value
            for out, them in sends:
                remote(
                    peaks.at[kind, them], peaks.at[kind, them], peak_send.at[kind, 0],
                    peak_recv.at[kind, them], x_dev,
                ).wait_recv()
                top = jnp.maximum(top, peaks[kind, them])
            return top

        return finish, [out for out, _ in sends]

    def tile_top(j, m):
        x = jnp.abs(raw_own[j]).reshape(-1, 4 * BLOCK, LANES)
        return jnp.maximum(m, jnp.max(x, axis=0))

    w_top = lax.fori_loop(0, tiles, tile_top, jnp.zeros((4 * BLOCK, LANES), jnp.bfloat16))
    w_top = jnp.full((8, LANES), jnp.max(w_top.astype(jnp.float32)), jnp.float32)

    def sib(s):
        return (s // 2) * 2 + 1 - s % 2

    finish_w, w_sends = peak_exchange(0, w_top, [(sib, 0), (0, 1), (sib, 1)])

    remote(kv_buf.at[far], kv_buf.at[far], kv_send.at[0], kv_recv.at[far], y_dev).wait_recv()
    kv_f.start()

    w_inv, w_scale = scales_of(finish_w()[0:1, :])

    def own_copy(p):
        sl = pl.ds(col0 + 2 * p, 2)
        return remote(w_own.at[sl], w_own.at[sl], own_send.at[p], own_recv.at[p], s_dev)

    def own_pair(p, c):
        for t in range(2):
            quant_tile(raw_own.at[2 * p + t], w_own.at[col0 + 2 * p + t], w_inv, w_scale)
        own_copy(p).start()
        return c

    lax.fori_loop(0, OWN_FIRST, own_pair, 0)
    forward(0)

    for c in q_loads:
        c.wait()
    for slot in (other, far_other):
        remote(kv_buf.at[slot], kv_buf.at[slot], kv_send.at[0], kv_recv.at[slot], s_dev).wait_recv()

    rate = HEAD_SIZE ** (-0.5)

    def scores_of(q, b):
        return lax.dot_general(
            q, kv_buf[b, 0], (((1,), (1,)), ((), ())), preferred_element_type=jnp.float32
        )

    def attend_tile(first, h):
        q = q_buf[h, pl.ds(first, share), :]
        s = scores_of(q, seq)
        row = lax.broadcasted_iota(jnp.int32, (share, tokens), 0) + first
        col = lax.broadcasted_iota(jnp.int32, (share, tokens), 1)
        s = jnp.where(row >= col, s, neg_large)
        top = jnp.max(s, axis=1, keepdims=True)
        p = jnp.exp((s - top) * rate)
        total = jnp.sum(p, axis=1, keepdims=True)
        acc = jnp.dot(p.astype(jnp.bfloat16), kv_buf[seq, 1], preferred_element_type=jnp.float32)

        def body(b, carry):
            top, total, acc = carry
            s = scores_of(q, b)
            new = jnp.maximum(top, jnp.max(s, axis=1, keepdims=True))
            fix = jnp.exp((top - new) * rate)
            p = jnp.exp((s - new) * rate)
            total = total * fix + jnp.sum(p, axis=1, keepdims=True)
            acc = acc * fix + jnp.dot(
                p.astype(jnp.bfloat16), kv_buf[b, 1], preferred_element_type=jnp.float32
            )
            return new, total, acc

        top, total, acc = lax.fori_loop(0, seq, body, (top, total, acc))
        out = (acc / total).astype(jnp.bfloat16)
        act_full[h, pl.ds(first, share), :] = out
        return jnp.max(jnp.abs(out.astype(jnp.float32)), axis=0, keepdims=True)

    theirs = pl.multiple_of((1 - tp) * share, share)
    mine = pl.multiple_of(tp * share, share)
    a_top = jnp.zeros((1, LANES), jnp.float32)

    def att_loop(first):
        def body(h, m):
            return jnp.maximum(m, attend_tile(first, h))

        return body

    a_top = lax.fori_loop(0, heads, att_loop(theirs), a_top)
    act_copy = remote(
        act_full.at[:, pl.ds(theirs, share), :], act_peer, act_sem.at[0], act_sem.at[1], x_dev
    )
    act_copy.start()
    forward(1)
    forward(2)
    a_top = lax.fori_loop(0, heads, att_loop(mine), a_top)
    a_top = jnp.full((8, LANES), jnp.max(a_top), jnp.float32)
    finish_a, a_sends = peak_exchange(1, a_top, team)

    forward(3)
    third = (pairs - OWN_FIRST) // 3
    lax.fori_loop(OWN_FIRST, OWN_FIRST + third, own_pair, 0)
    forward(4)
    lax.fori_loop(OWN_FIRST + third, OWN_FIRST + 2 * third, own_pair, 0)
    forward(5)
    lax.fori_loop(OWN_FIRST + 2 * third, pairs, own_pair, 0)
    for i in range(6, group):
        forward(i)

    a_inv, a_scale = scales_of(finish_a()[0:1, :])
    act_copy.wait_recv()
    spread = spread_matrix()
    for k in range(2):
        for h in range(heads):
            for lo in range(0, share, 64):
                if k == 0:
                    x = act_full[h, pl.ds(mine + lo, 64), :].astype(jnp.float32)
                else:
                    x = act_peer[h, lo : lo + 64, :].astype(jnp.float32)
                m = lane_block_max(jnp.abs(x))
                narrow = jnp.maximum(m * a_inv, scale_floor).astype(jnp.bfloat16)
                spacing = jnp.dot(narrow, spread, preferred_element_type=jnp.float32) * a_scale
                payload = soft_grid(x * (1.0 / spacing)).astype(jnp.bfloat16).astype(jnp.float32)
                act_q[k, lo : lo + 64, h * HEAD_SIZE : (h + 1) * HEAD_SIZE] = (
                    payload * spacing
                ).astype(jnp.bfloat16)

    square_sum[...] = jnp.zeros_like(square_sum)
    row_top[...] = jnp.zeros_like(row_top)

    def local_pair(p):
        late = p // (3 * group_pairs)
        sel = lax.rem(p, 3)
        fy = late + (1 - late) * (sel % 2)
        fz = late + (1 - late) * (sel // 2)
        g = lax.rem(y + fy, 2) + 2 * lax.rem(zz + fz, 2)
        i = (1 - late) * (p // 3) + late * (p - 3 * group_pairs)
        return g * group_pairs + i, late, sel, i

    def peer_copy(lp):
        sl = pl.ds(col0 + 2 * lp, 2)
        return remote(w_peer.at[sl], w_peer.at[sl], peer_send.at[lp], peer_recv.at[lp], s_dev)

    def out_copy(n):
        cols = pl.ds(pl.multiple_of(2 * n * LANES, 2 * LANES), 2 * LANES)
        return pltpu.make_async_copy(hid_buf.at[:, cols], hid_hbm.at[:, cols], out_sem.at[n])

    def project_pair(n):
        cols = pl.ds(pl.multiple_of(2 * n * LANES, 2 * LANES), 2 * LANES)
        a = jnp.concatenate([w_own[2 * n], w_own[2 * n + 1]], axis=1)
        b = jnp.concatenate([w_peer[2 * n], w_peer[2 * n + 1]], axis=1)
        part_own[...] = jnp.dot(act_q[0], a, preferred_element_type=jnp.float32)
        part_peer[...] = jnp.dot(act_q[1], b, preferred_element_type=jnp.float32)
        gain = gain_ref[:, cols]
        for lo in range(0, share, 32):
            p0 = part_own[lo : lo + 32, :].astype(jnp.bfloat16).astype(jnp.float32)
            p1 = part_peer[lo : lo + 32, :].astype(jnp.bfloat16).astype(jnp.float32)
            h = res_buf[lo : lo + 32, cols].astype(jnp.float32) + (p0 + p1)
            hid_buf[lo : lo + 32, cols] = h
            s = jnp.abs(h * gain)
            h = h * h
            square_sum[lo : lo + 32, :] += h[:, :LANES] + h[:, LANES:]
            row_top[lo : lo + 32, :] = jnp.maximum(
                row_top[lo : lo + 32, :], jnp.maximum(s[:, :LANES], s[:, LANES:])
            )
        out_copy(n).start()

    other0 = (1 - core) * tiles

    def sibling_pair(lp):
        sl = pl.ds(other0 + 2 * lp, 2)
        remote(w_own.at[sl], w_own.at[sl], own_send.at[0], own_recv.at[lp], s_dev).wait_recv()
        remote(w_peer.at[sl], w_peer.at[sl], peer_send.at[0], peer_recv.at[lp], s_dev).wait_recv()
        project_pair(other0 // 2 + lp)

    res_load.wait()

    def step(p, c):
        lp, late, sel, i = local_pair(p)

        @pl.when(late + sel > 0)
        def _():
            wait_tile(2 * lp)
            wait_tile(2 * lp + 1)

        @pl.when((1 - late) * sel * (sel % 2) * (2 * i // (relay_x + relay_y)) > 0)
        def _():
            for t in range(2):
                n = 2 * i + t - relay_x - relay_y
                z_send(group + n, 2 * lp + t).start()

        for lo in range(relay_x // 2, (relay_x + relay_y) // 2):
            @pl.when((1 - late) * (sel // 2) * (1 - (i - lo) * (i - lo)) > 0)
            def _():
                for t in range(2):
                    n = 2 * (lo - relay_x // 2) + t
                    y_send(group + n, 2 * lp + t).start()

        for t in range(2):
            quant_tile(raw_peer.at[2 * lp + t], w_peer.at[col0 + 2 * lp + t], w_inv, w_scale)
        peer_copy(lp).start()
        project_pair(col0 // 2 + lp)

        @pl.when(p > 0)
        def _():
            sibling_pair(local_pair(p - 1)[0])

        return c

    lax.fori_loop(0, pairs, step, 0)
    sibling_pair(local_pair(pairs - 1)[0])

    mean_square = jnp.sum(square_sum[...], axis=1, keepdims=True) / features
    rstd = lax.rsqrt(mean_square + 1e-05)
    rstd_ref[...] = jnp.broadcast_to(rstd, rstd_ref.shape)
    n_top = jnp.max(jnp.max(row_top[...], axis=1, keepdims=True) * rstd)
    finish_n, n_sends = peak_exchange(2, jnp.full((8, LANES), n_top, jnp.float32), team)

    kv_y.wait_send()
    kv_s.wait_send()
    kv_f.wait_send()
    act_copy.wait_send()
    for c in w_sends + a_sends:
        c.wait_send()

    def drain(n, c):
        own_copy(n).wait_send()
        peer_copy(n).wait_send()
        out_copy(n).wait()
        out_copy(n + pairs).wait()
        return c

    lax.fori_loop(0, pairs, drain, 0)

    def drain_links(i, c):
        remote(raw_own.at[0], raw_peer.at[0], x_sem.at[i], recv_sem.at[0], x_dev).wait_send()
        y_send(i, 0).wait_send()
        return c

    lax.fori_loop(0, x_count, drain_links, 0)

    def drain_z(i, c):
        z_send(i, 0).wait_send()
        return c

    lax.fori_loop(0, z_count, drain_z, 0)
    top_ref[...] = finish_n()
    for c in n_sends:
        c.wait_send()


def fused(queries, keys, values, out_weight, residual, gain):
    tokens, n_feat = queries.shape
    share, d = residual.shape
    heads = n_feat // HEAD_SIZE
    tiles = d // LANES // 2
    pairs = tiles // 2
    group = tiles // 4
    any_spec = pl.BlockSpec(memory_space=pl.ANY)
    vmem = pl.BlockSpec(memory_space=pltpu.VMEM)
    dma = pltpu.SemaphoreType.DMA
    bf16, f32 = jnp.bfloat16, jnp.float32
    rows = out_weight.shape[0]
    return pl.pallas_call(
        functools.partial(fused_kernel, features=d),
        in_specs=[any_spec] * 5 + [vmem],
        out_specs=[any_spec, vmem, vmem],
        out_shape=[
            jax.ShapeDtypeStruct((share, d), f32),
            jax.ShapeDtypeStruct((share, LANES), f32),
            jax.ShapeDtypeStruct((8, LANES), f32),
        ],
        scratch_shapes=[
            pltpu.VMEM((heads, tokens, HEAD_SIZE), bf16),
            pltpu.VMEM((4, 2, tokens, HEAD_SIZE), bf16),
            pltpu.VMEM((tiles, rows, LANES), bf16),
            pltpu.VMEM((tiles, rows, LANES), bf16),
            pltpu.VMEM((2 * tiles, rows, LANES), bf16),
            pltpu.VMEM((2 * tiles, rows, LANES), bf16),
            pltpu.VMEM((share, d), bf16),
            pltpu.VMEM((share, d), f32),
            pltpu.VMEM((heads, tokens, HEAD_SIZE), bf16),
            pltpu.VMEM((heads, share, HEAD_SIZE), bf16),
            pltpu.VMEM((2, share, n_feat), bf16),
            pltpu.VMEM((share, LANES), f32),
            pltpu.VMEM((share, LANES), f32),
            pltpu.VMEM((3, 8, 8, LANES), f32),
            pltpu.VMEM((share, 2 * LANES), f32),
            pltpu.VMEM((share, 2 * LANES), f32),
            dma((3 + heads,)),
            dma((tiles,)),
            dma((tiles,)),
            dma((group + group // 4,)),
            dma((group + group // 4,)),
            dma((2 * group - 2 * (group // 4),)),
            dma((3,)),
            dma((4,)),
            dma((3, 7)),
            dma((3, 8)),
            dma((2,)),
            dma((pairs,)),
            dma((pairs,)),
            dma((pairs,)),
            dma((pairs,)),
            dma((2 * pairs,)),
        ],
        compiler_params=pltpu.CompilerParams(
            collective_id=0, has_side_effects=True, vmem_limit_bytes=60 * 1024 * 1024
        ),
        name="fused",
    )(queries, keys, values, out_weight, residual, gain)


def final_fast_kernel(top_ref, hid_ref, rstd_ref, gain_ref, new_ref, out_ref, narrow, wide):
    rows, cols = hid_ref.shape
    inv, tensor_scale = scales_of(top_ref[0:1, :])
    spread = spread_matrix()
    rstd = rstd_ref[...]
    pieces = cols // LANES
    for i in range(pieces):
        sl = slice(i * LANES, (i + 1) * LANES)
        h = hid_ref[:, sl]
        new_ref[:, sl] = h.astype(jnp.bfloat16)
        m = lane_block_max(jnp.abs(h * rstd * gain_ref[:, sl]))
        narrow[i * rows : (i + 1) * rows, :] = jnp.maximum(m * inv, scale_floor).astype(jnp.bfloat16)
    wide[...] = jnp.dot(narrow[...], spread, preferred_element_type=jnp.float32)
    for i in range(pieces):
        sl = slice(i * LANES, (i + 1) * LANES)
        x = hid_ref[:, sl] * rstd * gain_ref[:, sl]
        spacing = wide[i * rows : (i + 1) * rows, :] * tensor_scale
        payload = soft_grid(x * pl.reciprocal(spacing)).astype(jnp.bfloat16).astype(jnp.float32)
        out_ref[:, sl] = (payload * spacing).astype(jnp.bfloat16)


def final_fast(top, hidden, rstd, gain):
    tokens, d = hidden.shape
    width, rows = 2048, 64
    column = pl.BlockSpec((rows, width), lambda i, j: (i, j))
    return pl.pallas_call(
        final_fast_kernel,
        grid=(tokens // rows, d // width),
        in_specs=[
            pl.BlockSpec((8, LANES), lambda i, j: (0, 0)),
            column,
            pl.BlockSpec((rows, LANES), lambda i, j: (i, 0)),
            pl.BlockSpec((1, width), lambda i, j: (0, j)),
        ],
        out_specs=[column, column],
        out_shape=[jax.ShapeDtypeStruct((tokens, d), jnp.bfloat16)] * 2,
        scratch_shapes=[
            pltpu.VMEM((rows * width // LANES, LANES), jnp.bfloat16),
            pltpu.VMEM((rows * width // LANES, LANES), jnp.float32),
        ],
        name="final_fast",
    )(top, hidden, rstd, gain)


def fits_fused(queries, keys, out_weight, residual):
    sizes = {a: lax.axis_size(a) for a in ("dp", "seq", "tp")}
    return (
        sizes["tp"] == 2
        and sizes["seq"] == 4
        and sizes["dp"] % 2 == 0
        and keys.shape[1] == HEAD_SIZE
        and out_weight.shape[1] % (64 * LANES) == 0
        and out_weight.shape[0] == queries.shape[1]
        and out_weight.shape[0] % LANES == 0
        and residual.shape[0] * 2 == queries.shape[0]
        and residual.shape[0] % 64 == 0
    )


def local(queries, keys, values, out_weight, residual, norm_gain):
    if not fits_fused(queries, keys, out_weight, residual):
        return general(queries, keys, values, out_weight, residual, norm_gain)
    gain = norm_gain.astype(jnp.float32).reshape(1, -1)
    hidden, rstd, top = fused(queries, keys, values, out_weight, residual, gain)
    return tuple(final_fast(top, hidden, rstd, gain))


def solution(mesh):
    in_specs = (
        P(("dp", "seq"), "tp"),
        P(("dp", "seq"), "tp"),
        P(("dp", "seq"), "tp"),
        P("tp", None),
        P(("dp", "seq", "tp"), None),
        P(),
    )
    out_specs = (P(("dp", "seq", "tp"), None), P(("dp", "seq", "tp"), None))
    return jax.shard_map(local, mesh=mesh, in_specs=in_specs, out_specs=out_specs, check_vma=False)
```

```python
import functools

import jax
import jax.numpy as jnp
import numpy as np
from jax import lax
from jax.experimental import pallas as pl
from jax.experimental.pallas import tpu as pltpu
from jax.sharding import PartitionSpec as P

HEAD_SIZE = 128
BLOCK = 16
softness = 0.9
scale_floor = 256.0
neg_large = -1e30
LANES = 128
AHEAD = 2
RAW = 2
ROUND_BIG = 25165824.0
Q_COEFFS = (0.8999997814, -0.5804296733, 0.1500389216, -0.0212977078, 0.0016888914)


def soft_grid(u):
    t = u - ((u + ROUND_BIG) - ROUND_BIG)
    z = t * t
    q = jnp.float32(Q_COEFFS[-1])
    for c in Q_COEFFS[-2::-1]:
        q = q * z + jnp.float32(c)
    return u - (t - t * z) * q


def spacing_of(block_max, peak):
    tensor_scale = peak / (6.0 * 448.0)
    inv = 1.0 / (6.0 * tensor_scale)
    scale = jnp.maximum(block_max * inv, scale_floor).astype(jnp.bfloat16)
    return scale, tensor_scale


def quant_rows(x, peak):
    rows, cols = x.shape
    xb = x.reshape(rows // BLOCK, BLOCK, cols)
    block_max = jnp.max(jnp.abs(xb), axis=1, keepdims=True)
    scale, tensor_scale = spacing_of(block_max, peak)
    spacing = scale.astype(jnp.float32) * tensor_scale
    payload = soft_grid(xb * (1.0 / spacing)).astype(jnp.bfloat16).astype(jnp.float32)
    return (payload * spacing).reshape(rows, cols)


def quant_kernel(peak_ref, w_ref, out_ref, *, unroll):
    peak = peak_ref[0, 0]
    rows = w_ref.shape[0]

    def step(i, carry):
        sl = pl.ds(pl.multiple_of(i * BLOCK, BLOCK), BLOCK)
        out_ref[sl, :] = quant_rows(w_ref[sl, :].astype(jnp.float32), peak).astype(jnp.bfloat16)
        return carry

    lax.fori_loop(0, rows // BLOCK, step, 0, unroll=unroll)


def quant_weight(w, peak, width, first, cols):
    rows = w.shape[0]
    skip = first // width
    return pl.pallas_call(
        functools.partial(quant_kernel, unroll=4),
        grid=(cols // width,),
        in_specs=[
            pl.BlockSpec(memory_space=pltpu.SMEM),
            pl.BlockSpec((rows, width), lambda i: (0, i + skip)),
        ],
        out_specs=pl.BlockSpec((rows, width), lambda i: (0, i)),
        out_shape=jax.ShapeDtypeStruct((rows, cols), jnp.bfloat16),
        cost_estimate=pl.CostEstimate(
            flops=40 * rows * cols, bytes_accessed=4 * rows * cols, transcendentals=0
        ),
        name="quant_weight",
    )(peak, w)


def project_kernel(*refs, n_tp, n_feat, n_alias, features):
    peak_ref, act_refs = refs[0], refs[1 : 1 + n_tp]
    own_ref, peer_ref, res_ref, gain_ref, sq_in, top_in = refs[1 + n_tp : 7 + n_tp]
    refs = refs[7 + n_tp + n_alias :]
    new_ref, hid_ref, square_sum, row_top, rstd_ref, top_ref, act_q = refs
    step_id = pl.program_id(0)

    @pl.when(step_id == 0)
    def _():
        peak = peak_ref[0, 0]
        square_sum[...] = sq_in[...]
        row_top[...] = top_in[...]
        for k in range(n_tp):
            for lo in range(0, n_feat, 128):
                x = act_refs[k][lo : lo + 128, :].astype(jnp.float32)
                act_q[k, :, lo : lo + 128] = quant_rows(x, peak).T.astype(jnp.bfloat16)

    hidden = res_ref[...].astype(jnp.float32)
    for k in range(n_tp):
        w = own_ref[...] if k == 0 else peer_ref[0, k - 1]
        part = jnp.dot(act_q[k], w, preferred_element_type=jnp.float32)
        hidden = hidden + part.astype(jnp.bfloat16).astype(jnp.float32)
    new_ref[...] = hidden.astype(jnp.bfloat16)
    hid_ref[...] = hidden
    sq = square_sum[...]
    top = row_top[...]
    scaled = jnp.abs(hidden * gain_ref[...])
    for lo in range(0, hidden.shape[1], 128):
        part = hidden[:, lo : lo + 128]
        sq = sq + part * part
        top = jnp.maximum(top, scaled[:, lo : lo + 128])
    square_sum[...] = sq
    row_top[...] = top

    @pl.when(step_id == pl.num_programs(0) - 1)
    def _():
        mean_square = jnp.sum(square_sum[...], axis=1, keepdims=True) / features
        rstd = lax.rsqrt(mean_square + 1e-05)
        rstd_ref[...] = jnp.broadcast_to(rstd, rstd_ref.shape)
        top_all = jnp.max(jnp.max(row_top[...], axis=1, keepdims=True) * rstd)
        top_ref[...] = jnp.full(top_ref.shape, top_all, jnp.float32)


def project(peak, acts, w_own, w_peer, residual, gain, stats, width, skip, wide, made):
    n_tp = len(acts)
    n_feat, tokens = acts[0].shape
    d = residual.shape[1]
    steps = w_own.shape[1] // width
    column = pl.BlockSpec((tokens, width), lambda i: (0, i + skip))
    whole = pl.BlockSpec((tokens, 128), lambda i: (0, 0))
    if wide:
        peer_spec = pl.BlockSpec((1, n_tp - 1, n_feat, width), lambda i: (0, 0, 0, i))
    else:
        peer_spec = pl.BlockSpec((1, n_tp - 1, n_feat, width), lambda i: (i, 0, 0, 0))
    stat = jax.ShapeDtypeStruct((tokens, 128), jnp.float32)
    return pl.pallas_call(
        functools.partial(project_kernel, n_tp=n_tp, n_feat=n_feat, n_alias=len(made), features=d),
        grid=(steps,),
        in_specs=[pl.BlockSpec(memory_space=pltpu.SMEM)]
        + [pl.BlockSpec((n_feat, tokens), lambda i: (0, 0))] * n_tp
        + [
            pl.BlockSpec((n_feat, width), lambda i: (0, i)),
            peer_spec,
            column,
            pl.BlockSpec((1, width), lambda i: (0, i + skip)),
            whole,
            whole,
        ]
        + [pl.BlockSpec(memory_space=pl.ANY)] * len(made),
        out_specs=[column, column, whole, whole, whole, pl.BlockSpec((8, 128), lambda i: (0, 0))],
        out_shape=[
            jax.ShapeDtypeStruct((tokens, d), jnp.bfloat16),
            jax.ShapeDtypeStruct((tokens, d), jnp.float32),
            stat,
            stat,
            stat,
            jax.ShapeDtypeStruct((8, 128), jnp.float32),
        ],
        input_output_aliases={7 + n_tp + i: i for i in range(len(made))},
        scratch_shapes=[pltpu.VMEM((n_tp, tokens, n_feat), jnp.bfloat16)],
        cost_estimate=pl.CostEstimate(
            flops=2 * n_tp * n_feat * tokens * steps * width,
            bytes_accessed=2 * n_tp * n_feat * steps * width,
            transcendentals=0,
        ),
        name="project",
    )(peak, *acts, w_own, w_peer, residual, gain, *stats, *made)


def final_kernel(peak_ref, hid_ref, rstd_ref, gain_ref, out_ref, narrow, wide):
    peak = peak_ref[0, 0]
    rows, cols = hid_ref.shape
    src = lax.broadcasted_iota(jnp.int32, (128, 128), 0)
    dst = lax.broadcasted_iota(jnp.int32, (128, 128), 1)
    spread = jnp.where(src == (dst // BLOCK) * BLOCK + BLOCK - 1, 1.0, 0.0).astype(jnp.bfloat16)
    rstd = rstd_ref[...]
    tensor_scale = peak / (6.0 * 448.0)
    pieces = cols // 128
    for i in range(pieces):
        x = hid_ref[:, i * 128 : i * 128 + 128] * rstd * gain_ref[:, i * 128 : i * 128 + 128]
        m = jnp.abs(x)
        for s in (1, 2, 4, 8):
            m = jnp.maximum(m, pltpu.roll(m, s, 1))
        narrow[i * rows : (i + 1) * rows, :] = spacing_of(m, peak)[0]
    wide[...] = jnp.dot(narrow[...], spread, preferred_element_type=jnp.float32)
    for i in range(pieces):
        x = hid_ref[:, i * 128 : i * 128 + 128] * rstd * gain_ref[:, i * 128 : i * 128 + 128]
        spacing = wide[i * rows : (i + 1) * rows, :] * tensor_scale
        payload = soft_grid(x * pl.reciprocal(spacing)).astype(jnp.bfloat16).astype(jnp.float32)
        out_ref[:, i * 128 : i * 128 + 128] = (payload * spacing).astype(jnp.bfloat16)


def final_quant(peak, hidden, rstd, gain):
    tokens, d = hidden.shape
    width = 2048
    rows = min(64, tokens)
    column = pl.BlockSpec((rows, width), lambda i, j: (i, j))
    return pl.pallas_call(
        final_kernel,
        grid=(tokens // rows, d // width),
        in_specs=[
            pl.BlockSpec(memory_space=pltpu.SMEM),
            column,
            pl.BlockSpec((rows, 128), lambda i, j: (i, 0)),
            pl.BlockSpec((1, width), lambda i, j: (0, j)),
        ],
        out_specs=column,
        out_shape=jax.ShapeDtypeStruct((tokens, d), jnp.bfloat16),
        scratch_shapes=[
            pltpu.VMEM((rows * width // 128, 128), jnp.bfloat16),
            pltpu.VMEM((rows * width // 128, 128), jnp.float32),
        ],
        name="final_quant",
    )(peak, hidden, rstd, gain)


def attend(queries, keys, values, first_query):
    token_count = queries.shape[0]
    kv_heads = keys.shape[1] // HEAD_SIZE
    grouped = queries.shape[1] // HEAD_SIZE // kv_heads
    q = queries.reshape(token_count, kv_heads, grouped, HEAD_SIZE)
    k = keys.reshape(-1, kv_heads, HEAD_SIZE)
    v = values.reshape(-1, kv_heads, HEAD_SIZE)
    scores = jnp.einsum("tkgd,skd->kgts", q, k, preferred_element_type=jnp.float32)
    scores = scores * HEAD_SIZE ** (-0.5)
    query_pos = first_query + lax.broadcasted_iota(jnp.int32, (token_count, 1), 0)
    key_pos = lax.broadcasted_iota(jnp.int32, (1, k.shape[0]), 1)
    allowed = query_pos >= key_pos
    masked = jnp.where(allowed, scores, neg_large)
    top = jnp.max(masked, axis=3, keepdims=True)
    weights = jnp.where(allowed, jnp.exp(masked - top), 0.0)
    total = jnp.sum(weights, axis=3)
    summed = jnp.einsum(
        "kgts,skd->kgtd", weights.astype(jnp.bfloat16), v, preferred_element_type=jnp.float32
    )
    attended = (summed / total[..., None]).astype(jnp.bfloat16)
    return attended.transpose(0, 1, 3, 2).reshape(-1, token_count)


def general(queries, keys, values, out_weight, residual, norm_gain):
    token_count = queries.shape[0]
    n_tp = lax.axis_size("tp")
    tp_rank = lax.axis_index("tp")
    slabs = lax.axis_size("dp") * lax.axis_size("seq")
    d = out_weight.shape[1]
    width = d // slabs
    kv = lax.all_gather(jnp.stack((keys, values)), "seq", axis=1, tiled=True)

    weight_top = jnp.max(jnp.abs(out_weight)).astype(jnp.float32)
    weight_peak = lax.pmax(weight_top, "tp").reshape(1, 1)
    slab_id = lax.axis_index("dp") * lax.axis_size("seq") + lax.axis_index("seq")
    direct = 128
    gather_w = width - direct
    gathered = slabs * gather_w
    slab = lax.dynamic_slice_in_dim(out_weight, slab_id * gather_w, gather_w, axis=1)
    slab_q = quant_weight(slab, weight_peak, gather_w, 0, gather_w)
    shifts = [[(i, (i + k) % n_tp) for i in range(n_tp)] for k in range(1, n_tp)]
    from_peers = jnp.stack([lax.ppermute(slab_q, "tp", ring) for ring in shifts])
    w_peer = lax.all_gather(from_peers, ("dp", "seq"), axis=0)
    near_own = quant_weight(out_weight, weight_peak, 512, gathered, d - gathered)
    near_peer = jnp.stack([lax.ppermute(near_own, "tp", ring) for ring in shifts])[None]
    w_own = quant_weight(out_weight, weight_peak, gather_w, 0, gathered)

    act_t = attend(queries, kv[0], kv[1], lax.axis_index("seq") * token_count)
    act_top = jnp.max(jnp.abs(act_t)).astype(jnp.float32)
    share = token_count // n_tp
    pieces = []
    for k in range(n_tp):
        whose = lax.rem(tp_rank + k, n_tp)
        piece = lax.dynamic_slice_in_dim(act_t, whose * share, share, axis=1)
        pieces.append(piece if k == 0 else lax.ppermute(piece, "tp", shifts[k - 1]))
    act_peak = lax.pmax(act_top, ("seq", "tp")).reshape(1, 1)

    gain = norm_gain.astype(jnp.float32).reshape(1, d)
    stats = (jnp.zeros((share, 128), jnp.float32),) * 2
    near = project(
        act_peak, pieces, near_own, near_peer, residual, gain, stats, 512, gathered // 512, True, ()
    )
    new_residual, hidden, _, _, rstd, top = project(
        act_peak, pieces, w_own, w_peer, residual, gain, near[2:4], gather_w, 0, False, near[:2]
    )
    norm_peak = lax.pmax(top[0, 0], ("seq", "tp")).reshape(1, 1)
    next_input = final_quant(norm_peak, hidden, rstd, gain)
    return (new_residual, next_input)


def quant_tile(src, dst, inv, tensor_scale):
    rows = src.shape[0]
    step = 128 if rows % 128 == 0 else BLOCK
    for lo in range(0, rows, step):
        x = src[lo : lo + step, :].astype(jnp.float32).reshape(step // BLOCK, BLOCK, LANES)
        block_max = jnp.max(jnp.abs(x), axis=1, keepdims=True)
        scale = jnp.maximum(block_max * inv, scale_floor).astype(jnp.bfloat16)
        spacing = scale.astype(jnp.float32) * tensor_scale
        payload = soft_grid(x * (1.0 / spacing)).astype(jnp.bfloat16).astype(jnp.float32)
        dst[lo : lo + step, :] = (payload * spacing).reshape(step, LANES).astype(jnp.bfloat16)


def scales_of(top):
    tensor_scale = top / (6.0 * 448.0)
    return 1.0 / (6.0 * tensor_scale), tensor_scale


def lane_block_max(m):
    for s in (1, 2, 4, 8):
        m = jnp.maximum(m, pltpu.roll(m, s, 1))
    return m


def spread_matrix():
    src = lax.broadcasted_iota(jnp.int32, (LANES, LANES), 0)
    dst = lax.broadcasted_iota(jnp.int32, (LANES, LANES), 1)
    return jnp.where(src == (dst // BLOCK) * BLOCK + BLOCK - 1, 1.0, 0.0).astype(jnp.bfloat16)


def fused_kernel(
    q_hbm, k_hbm, v_hbm, w_hbm, res_hbm, gain_ref,
    hid_hbm, rstd_ref, top_ref, bm_ref,
    q_buf, kv_buf, raw_own, raw_peer, w_own, w_peer, res_buf, hid_buf,
    act_full, act_peer, act_q, square_sum, peaks,
    local_sem, load_sem, recv_sem, x_sem, y_sem, z_sem,
    kv_send, kv_recv, peak_send, peak_recv, act_sem,
    own_send, own_recv, peer_send, peer_recv, out_sem,
    *, features,
):
    tokens = k_hbm.shape[0]
    heads = q_hbm.shape[1] // HEAD_SIZE
    share = res_hbm.shape[0]
    n_feat = heads * HEAD_SIZE
    tiles = raw_own.shape[0]
    group = tiles // 4
    pairs = tiles // 2
    group_pairs = group // 2
    direct = group // 4
    relays = group - direct
    dp, seq, tp = lax.axis_index("dp"), lax.axis_index("seq"), lax.axis_index("tp")
    core, y = seq % 2, seq // 2
    zz = dp % 2
    x_dev = {"dp": dp, "seq": seq, "tp": 1 - tp}
    y_dev = {"dp": dp, "seq": (1 - y) * 2 + core, "tp": tp}
    z_dev = {"dp": dp + 1 - 2 * zz, "seq": seq, "tp": tp}
    s_dev = {"dp": dp, "seq": y * 2 + 1 - core, "tp": tp}

    def remote(src, dst, send, recv, dev):
        return pltpu.make_async_remote_copy(
            src_ref=src, dst_ref=dst, send_sem=send, recv_sem=recv,
            device_id=dev, device_id_type=pl.DeviceIdType.MESH,
        )

    g_mine, g_y = y + 2 * zz, (1 - y) + 2 * zz
    g_z, g_d = y + 2 * (1 - zz), (1 - y) + 2 * (1 - zz)
    x_count = group + direct
    y_count = group + relays // 2

    col0 = core * tiles

    def tile_of(j, raw):
        return raw_peer.at[j] if raw else w_peer.at[col0 + j]

    def x_send(i):
        j = g_mine * group + i if i < group else g_d * group + relays + i - group
        src = raw_own.at[j] if i < RAW else w_own.at[col0 + j]
        return remote(src, tile_of(j, i < RAW), x_sem.at[i], recv_sem.at[j], x_dev)

    def y_send(i, j, raw=False):
        return remote(tile_of(j, raw), tile_of(j, raw), y_sem.at[i], recv_sem.at[j], y_dev)

    def z_send(i, j, raw=False):
        return remote(tile_of(j, raw), tile_of(j, raw), z_sem.at[i], recv_sem.at[j], z_dev)

    def wait_tile(j):
        remote(raw_peer.at[j], raw_peer.at[j], x_sem.at[0], recv_sem.at[j], x_dev).wait_recv()

    def forward(i):
        j = g_mine * group + i
        wait_tile(j)
        y_send(i, j, i < RAW).start()
        z_send(i, j, i < RAW).start()
        if i + AHEAD < x_count:
            x_send(i + AHEAD).start()

    def relay(t):
        if t % 2 == 0:
            j = g_z * group + t
            wait_tile(j)
            y_send(group + t // 2, j, t < RAW).start()
        else:
            j = g_y * group + t
            wait_tile(j)
            z_send(group + t // 2, j, t < RAW).start()

    def load(j):
        cols = pl.ds(pl.multiple_of((col0 + j) * LANES, LANES), LANES)
        return pltpu.make_async_copy(w_hbm.at[:, cols], raw_own.at[j], load_sem.at[j])

    k_load = pltpu.make_async_copy(k_hbm, kv_buf.at[seq, 0], local_sem.at[0])
    v_load = pltpu.make_async_copy(v_hbm, kv_buf.at[seq, 1], local_sem.at[1])
    res_load = pltpu.make_async_copy(res_hbm, res_buf, local_sem.at[2])
    q_loads = [
        pltpu.make_async_copy(
            q_hbm.at[:, h * HEAD_SIZE : (h + 1) * HEAD_SIZE], q_buf.at[h], local_sem.at[3 + h]
        )
        for h in range(heads)
    ]

    def load_order(n):
        return lax.rem(g_mine * group + n, tiles)

    def start_load(n, c):
        load(load_order(n)).start()
        return c

    k_load.start()
    v_load.start()
    lax.fori_loop(0, tiles, start_load, 0)
    for c in q_loads:
        c.start()
    res_load.start()

    barrier = pltpu.get_barrier_semaphore()
    team = []
    for ds in range(4):
        for dt in range(2):
            if ds or dt:
                team.append((ds, dt))
    for ds, dt in team:
        dev = {"dp": dp, "seq": lax.rem(seq + ds, 4), "tp": lax.rem(tp + dt, 2)}
        pl.semaphore_signal(barrier, inc=1, device_id=dev, device_id_type=pl.DeviceIdType.MESH)
    pl.semaphore_signal(barrier, inc=1, device_id=z_dev, device_id_type=pl.DeviceIdType.MESH)
    pl.semaphore_wait(barrier, len(team) + 1)

    k_load.wait()
    v_load.wait()
    other = y * 2 + 1 - core
    far = (1 - y) * 2 + core
    far_other = (1 - y) * 2 + 1 - core
    kv_y = remote(kv_buf.at[seq], kv_buf.at[seq], kv_send.at[0], kv_recv.at[seq], y_dev)
    kv_s = remote(kv_buf.at[seq], kv_buf.at[seq], kv_send.at[1], kv_recv.at[seq], s_dev)
    kv_f = remote(kv_buf.at[far], kv_buf.at[far], kv_send.at[2], kv_recv.at[far], s_dev)
    kv_y.start()
    kv_s.start()

    def wait_load(n, c):
        load(load_order(n)).wait()
        return c

    lax.fori_loop(0, tiles, wait_load, 0)

    def peak_exchange(kind, value, members):
        me = seq * 2 + tp
        peaks[kind, me] = value
        sends = []
        for ds, dt in members:
            ps = ds(seq) if callable(ds) else lax.rem(seq + ds, 4)
            pt = lax.rem(tp + dt, 2)
            dev = {"dp": dp, "seq": ps, "tp": pt}
            n = len(sends)
            out = remote(
                peaks.at[kind, me], peaks.at[kind, me], peak_send.at[kind, n],
                peak_recv.at[kind, me], dev,
            )
            out.start()
            sends.append((out, ps * 2 + pt))

        def finish():
            top = value
            for out, them in sends:
                remote(
                    peaks.at[kind, them], peaks.at[kind, them], peak_send.at[kind, 0],
                    peak_recv.at[kind, them], x_dev,
                ).wait_recv()
                top = jnp.maximum(top, peaks[kind, them])
            return top

        return finish, [out for out, _ in sends]

    def tile_top(j, m):
        x = jnp.abs(raw_own[pl.ds(4 * j, 4)]).reshape(-1, 8 * BLOCK, LANES)
        return jnp.maximum(m, jnp.max(x, axis=0))

    w_top = lax.fori_loop(0, tiles // 4, tile_top, jnp.zeros((8 * BLOCK, LANES), jnp.bfloat16))
    w_top = jnp.full((8, LANES), jnp.max(w_top.astype(jnp.float32)), jnp.float32)

    def sib(s):
        return (s // 2) * 2 + 1 - s % 2

    finish_w, w_sends = peak_exchange(0, w_top, [(sib, 0), (0, 1), (sib, 1)])

    for i in range(RAW):
        x_send(i).start()
    w_inv, w_scale = scales_of(finish_w()[0:1, :])

    def own_copy(p):
        sl = pl.ds(col0 + 2 * p, 2)
        return remote(w_own.at[sl], w_own.at[sl], own_send.at[p], own_recv.at[p], s_dev)

    def own_pair(p):
        for t in range(2):
            quant_tile(raw_own.at[2 * p + t], w_own.at[col0 + 2 * p + t], w_inv, w_scale)
        own_copy(p).start()

    def own_range(first, count):
        def body(n, c):
            own_pair(first + n)
            return c

        lax.fori_loop(0, count, body, 0)

    half = group_pairs
    own_range(g_mine * half + 1, half - 1)
    remote(kv_buf.at[far], kv_buf.at[far], kv_send.at[0], kv_recv.at[far], y_dev).wait_recv()
    kv_f.start()
    forward(0)

    for c in q_loads:
        c.wait()
    for slot in (other, far_other):
        remote(kv_buf.at[slot], kv_buf.at[slot], kv_send.at[0], kv_recv.at[slot], s_dev).wait_recv()

    rate = HEAD_SIZE ** (-0.5) * 1.4426950408889634

    def scores_of(q, b):
        return lax.dot_general(
            q, kv_buf[b, 0], (((1,), (1,)), ((), ())), preferred_element_type=jnp.float32
        )

    def weigh(p, b):
        return jnp.dot(p.astype(jnp.bfloat16), kv_buf[b, 1], preferred_element_type=jnp.float32)

    def attend_tiles(first, h0, m):
        qs = [q_buf[h0 + u, pl.ds(first, share), :] for u in range(2)]
        row = lax.broadcasted_iota(jnp.int32, (share, tokens), 0) + first
        col = lax.broadcasted_iota(jnp.int32, (share, tokens), 1)
        state = []
        for q in qs:
            s = jnp.where(row >= col, scores_of(q, seq), neg_large)
            top = jnp.max(s, axis=1, keepdims=True)
            p = jnp.exp2((s - top) * rate)
            state.append((top, jnp.sum(p, axis=1, keepdims=True), weigh(p, seq)))

        def body(b, state):
            out = []
            for q, (top, total, acc) in zip(qs, state):
                s = scores_of(q, b)
                new = jnp.maximum(top, jnp.max(s, axis=1, keepdims=True))
                fix = jnp.exp2((top - new) * rate)
                p = jnp.exp2((s - new) * rate)
                total = total * fix + jnp.sum(p, axis=1, keepdims=True)
                out.append((new, total, acc * fix + weigh(p, b)))
            return tuple(out)

        for u, (top, total, acc) in enumerate(lax.fori_loop(0, seq, body, tuple(state))):
            out = (acc / total).astype(jnp.bfloat16)
            act_full[h0 + u, pl.ds(first, share), :] = out
            m = jnp.maximum(m, jnp.max(jnp.abs(out.astype(jnp.float32)), axis=0, keepdims=True))
        return m

    theirs = pl.multiple_of((1 - tp) * share, share)
    mine = pl.multiple_of(tp * share, share)
    a_top = jnp.zeros((1, LANES), jnp.float32)
    act_copy = remote(
        act_full.at[:, pl.ds(theirs, share), :], act_peer, act_sem.at[0], act_sem.at[1], x_dev
    )
    pieces = [(theirs, h) for h in range(0, heads, 2)] + [(mine, h) for h in range(0, heads, 2)]

    def att_piece(n, m):
        late = n // (heads // 2)
        first = pl.multiple_of((late * tp + (1 - late) * (1 - tp)) * share, share)
        return attend_tiles(first, 2 * lax.rem(n, heads // 2), m)

    a_top = lax.fori_loop(0, 1, att_piece, a_top)
    forward(1)
    a_top = lax.fori_loop(1, 2, att_piece, a_top)
    act_copy.start()
    forward(2)
    a_top = lax.fori_loop(2, 3, att_piece, a_top)
    relay(0)
    relay(1)
    a_top = lax.fori_loop(3, 4, att_piece, a_top)
    a_top = jnp.full((8, LANES), jnp.max(a_top), jnp.float32)
    finish_a, a_sends = peak_exchange(1, a_top, team)
    forward(3)
    relay(2)
    own_range(g_d * half + half - 1, 1)
    own_range(g_mine * half, 1)
    own_range(g_y * half, half)
    own_range(g_z * half, half)
    forward(4)
    relay(3)
    own_range(g_d * half, half - 1)
    square_sum[...] = jnp.zeros_like(square_sum)
    bm_ref[...] = jnp.zeros_like(bm_ref)

    def local_pair(p):
        late = p // (3 * group_pairs)
        sel = lax.rem(p, 3)
        fy = late + (1 - late) * (sel % 2)
        fz = late + (1 - late) * (sel // 2)
        g = lax.rem(y + fy, 2) + 2 * lax.rem(zz + fz, 2)
        i = (1 - late) * (p // 3) + late * (p - 3 * group_pairs)
        return g * group_pairs + i, late, sel, i

    def peer_copy(lp):
        sl = pl.ds(col0 + 2 * lp, 2)
        return remote(w_peer.at[sl], w_peer.at[sl], peer_send.at[lp], peer_recv.at[lp], s_dev)

    def take_raw(p):
        lp = local_pair(p)[0]
        if p == 3 * group_pairs:
            wait_tile(2 * lp)
            wait_tile(2 * lp + 1)
        elif p:
            wait_tile(2 * lp + p - 1)
        for t in range(2):
            quant_tile(raw_peer.at[2 * lp + t], w_peer.at[col0 + 2 * lp + t], w_inv, w_scale)
        peer_copy(lp).start()

    for p in (0, 1, 2, 3 * group_pairs):
        take_raw(p)
    forward(5)
    relay(4)

    a_inv, a_scale = scales_of(finish_a()[0:1, :])
    act_copy.wait_recv()
    spread = spread_matrix()
    for k in range(2):
        for h in range(heads):
            for lo in range(0, share, 64):
                if k == 0:
                    x = act_full[h, pl.ds(mine + lo, 64), :].astype(jnp.float32)
                else:
                    x = act_peer[h, lo : lo + 64, :].astype(jnp.float32)
                m = lane_block_max(jnp.abs(x))
                narrow = jnp.maximum(m * a_inv, scale_floor).astype(jnp.bfloat16)
                spacing = jnp.dot(narrow, spread, preferred_element_type=jnp.float32) * a_scale
                payload = soft_grid(x * (1.0 / spacing)).astype(jnp.bfloat16).astype(jnp.float32)
                act_q[k, lo : lo + 64, h * HEAD_SIZE : (h + 1) * HEAD_SIZE] = (
                    payload * spacing
                ).astype(jnp.bfloat16)

    def out_copy(n):
        cols = pl.ds(pl.multiple_of(2 * n * LANES, 2 * LANES), 2 * LANES)
        return pltpu.make_async_copy(hid_buf.at[:, cols], hid_hbm.at[:, cols], out_sem.at[n])

    lane = lax.broadcasted_iota(jnp.int32, (32, LANES), 1)
    odd = lane % 2 == 1

    def epilogue(n, own, peer):
        cols = pl.ds(pl.multiple_of(2 * n * LANES, 2 * LANES), 2 * LANES)
        gain = gain_ref[:, cols]
        mask = (lane // 2) % 8 == n % 8
        turns = [LANES - s + 2 * s * ((2 * n // s) % 2) for s in (2, 4, 8)]
        for lo in range(0, share, 32):
            p0 = own[lo : lo + 32, :].astype(jnp.bfloat16).astype(jnp.float32)
            p1 = peer[lo : lo + 32, :].astype(jnp.bfloat16).astype(jnp.float32)
            h = res_buf[lo : lo + 32, cols].astype(jnp.float32) + (p0 + p1)
            hid_buf[lo : lo + 32, cols] = h
            s = jnp.abs(h * gain)
            h = h * h
            square_sum[lo : lo + 32, :] += h[:, :LANES] + h[:, LANES:]
            m0, m1 = s[:, :LANES], s[:, LANES:]
            m0 = jnp.maximum(m0, pltpu.roll(m0, LANES - 1, 1))
            m1 = jnp.maximum(m1, pltpu.roll(m1, 1, 1))
            m = jnp.where(odd, m1, m0)
            for turn in turns:
                m = jnp.maximum(m, pltpu.roll(m, turn, 1))
            bm_ref[n // 8, lo : lo + 32, :] = jnp.where(mask, m, bm_ref[n // 8, lo : lo + 32, :])

    def product(k, w, n):
        w = jnp.concatenate([w[2 * n], w[2 * n + 1]], axis=1)
        return jnp.dot(act_q[k], w, preferred_element_type=jnp.float32)

    def project(pair_ids):
        parts = [(product(0, w_own, n), product(1, w_peer, n)) for n in pair_ids]
        for n, (own, peer) in zip(pair_ids, parts):
            epilogue(n, own, peer)
        for n in pair_ids:
            out_copy(n).start()

    other0 = (1 - core) * tiles

    def take(p):
        lp, late, sel, i = local_pair(p)

        @pl.when((1 - late) * sel * (i // (group_pairs - 1)) + late > 0)
        def _():
            wait_tile(2 * lp)
            wait_tile(2 * lp + 1)

        @pl.when((1 - late) * sel * (1 - i // (group_pairs - 1)) > 0)
        def _():
            wait_tile(2 * lp + sel - 1)

        peer_copy(lp).start()

    res_load.wait()
    forward(6)

    def step(p, c):
        @pl.when(p == 1)
        def _():
            relay(5)

        @pl.when(p == 2)
        def _():
            forward(7)

        @pl.when((p > 1) * (p < pairs - 1) * (p + 1 != 3 * group_pairs))
        def _():
            take(p + 1)

        lp = local_pair(p)[0]
        sl = pl.ds(other0 + 2 * lp, 2)
        remote(w_own.at[sl], w_own.at[sl], own_send.at[0], own_recv.at[lp], s_dev).wait_recv()
        remote(w_peer.at[sl], w_peer.at[sl], peer_send.at[0], peer_recv.at[lp], s_dev).wait_recv()
        project([col0 // 2 + lp, other0 // 2 + lp])
        return c

    lax.fori_loop(0, pairs, step, 0)

    mean_square = jnp.sum(square_sum[...], axis=1, keepdims=True) / features
    rstd = lax.rsqrt(mean_square + 1e-05)
    rstd_ref[...] = jnp.broadcast_to(rstd, rstd_ref.shape)
    n_top = jnp.max(jnp.max(bm_ref[...], axis=0) * rstd)
    finish_n, n_sends = peak_exchange(2, jnp.full((8, LANES), n_top, jnp.float32), team)

    kv_y.wait_send()
    kv_s.wait_send()
    kv_f.wait_send()
    act_copy.wait_send()
    for c in w_sends + a_sends:
        c.wait_send()

    def drain(n, c):
        own_copy(n).wait_send()
        peer_copy(n).wait_send()
        out_copy(n).wait()
        out_copy(n + pairs).wait()
        return c

    lax.fori_loop(0, pairs, drain, 0)

    def drain_x(i, c):
        remote(raw_own.at[0], raw_peer.at[0], x_sem.at[i], recv_sem.at[0], x_dev).wait_send()
        return c

    lax.fori_loop(0, x_count, drain_x, 0)

    def drain_yz(i, c):
        y_send(i, 0).wait_send()
        z_send(i, 0).wait_send()
        return c

    lax.fori_loop(0, y_count, drain_yz, 0)
    top_ref[...] = finish_n()
    for c in n_sends:
        c.wait_send()


def fused(queries, keys, values, out_weight, residual, gain):
    tokens, n_feat = queries.shape
    share, d = residual.shape
    heads = n_feat // HEAD_SIZE
    tiles = d // LANES // 2
    pairs = tiles // 2
    group = tiles // 4
    any_spec = pl.BlockSpec(memory_space=pl.ANY)
    vmem = pl.BlockSpec(memory_space=pltpu.VMEM)
    dma = pltpu.SemaphoreType.DMA
    bf16, f32 = jnp.bfloat16, jnp.float32
    rows = out_weight.shape[0]
    return pl.pallas_call(
        functools.partial(fused_kernel, features=d),
        in_specs=[any_spec] * 5 + [vmem],
        out_specs=[any_spec, vmem, vmem, vmem],
        out_shape=[
            jax.ShapeDtypeStruct((share, d), f32),
            jax.ShapeDtypeStruct((share, LANES), f32),
            jax.ShapeDtypeStruct((8, LANES), f32),
            jax.ShapeDtypeStruct((d // (BLOCK * LANES), share, LANES), f32),
        ],
        scratch_shapes=[
            pltpu.VMEM((heads, tokens, HEAD_SIZE), bf16),
            pltpu.VMEM((4, 2, tokens, HEAD_SIZE), bf16),
            pltpu.VMEM((tiles, rows, LANES), bf16),
            pltpu.VMEM((tiles, rows, LANES), bf16),
            pltpu.VMEM((2 * tiles, rows, LANES), bf16),
            pltpu.VMEM((2 * tiles, rows, LANES), bf16),
            pltpu.VMEM((share, d), bf16),
            pltpu.VMEM((share, d), f32),
            pltpu.VMEM((heads, tokens, HEAD_SIZE), bf16),
            pltpu.VMEM((heads, share, HEAD_SIZE), bf16),
            pltpu.VMEM((2, share, n_feat), bf16),
            pltpu.VMEM((share, LANES), f32),
            pltpu.VMEM((3, 8, 8, LANES), f32),
            dma((3 + heads,)),
            dma((tiles,)),
            dma((tiles,)),
            dma((group + group // 4,)),
            dma((group + 3 * group // 8,)),
            dma((group + 3 * group // 8,)),
            dma((3,)),
            dma((4,)),
            dma((3, 7)),
            dma((3, 8)),
            dma((2,)),
            dma((pairs,)),
            dma((pairs,)),
            dma((pairs,)),
            dma((pairs,)),
            dma((2 * pairs,)),
        ],
        compiler_params=pltpu.CompilerParams(
            collective_id=0, has_side_effects=True, vmem_limit_bytes=60 * 1024 * 1024
        ),
        name="fused",
    )(queries, keys, values, out_weight, residual, gain)


def two_parts(x):
    high = x.astype(jnp.bfloat16)
    low = (x - high.astype(jnp.float32)).astype(jnp.bfloat16)
    return jnp.concatenate([high, low], axis=1)


def final_fast_kernel(top_ref, hid_ref, rstd_ref, bm_ref, gain_ref, wide_ref, new_ref, out_ref):
    rows = hid_ref.shape[0]
    groups = bm_ref.shape[0]
    inv, tensor_scale = scales_of(top_ref[0:1, :])
    rstd = rstd_ref[...]
    rates, spacings = [], []
    for g in range(groups):
        scale = jnp.maximum(bm_ref[g] * rstd * inv, scale_floor).astype(jnp.bfloat16)
        spacing = scale.astype(jnp.float32) * tensor_scale
        rates.append(two_parts(rstd / spacing))
        spacings.append(two_parts(spacing))
    rates = jnp.concatenate(rates, axis=0)
    spacings = jnp.concatenate(spacings, axis=0)
    width = 2 * LANES
    for v in range(BLOCK // 2):
        wide = wide_ref[:, v * width : (v + 1) * width]
        rate = jnp.dot(rates, wide, preferred_element_type=jnp.float32)
        spacing = jnp.dot(spacings, wide, preferred_element_type=jnp.float32)
        for g in range(groups):
            lo = (g * BLOCK // 2 + v) * width
            h = hid_ref[:, lo : lo + width]
            new_ref[:, lo : lo + width] = h.astype(jnp.bfloat16)
            u = (h * gain_ref[:, lo : lo + width]) * rate[g * rows : (g + 1) * rows]
            payload = soft_grid(u).astype(jnp.bfloat16).astype(jnp.float32)
            out_ref[:, lo : lo + width] = (payload * spacing[g * rows : (g + 1) * rows]).astype(
                jnp.bfloat16
            )


def final_fast(top, hidden, rstd, block_max, gain):
    tokens, d = hidden.shape
    groups = block_max.shape[0]
    rows = 64
    src = np.arange(2 * LANES)[:, None] % LANES
    dst = np.arange(BLOCK * LANES)[None, :]
    wide = jnp.asarray(src == dst % LANES // BLOCK * BLOCK + dst // LANES, jnp.bfloat16)
    line = pl.BlockSpec((rows, d), lambda i: (i, 0))
    return pl.pallas_call(
        final_fast_kernel,
        grid=(tokens // rows,),
        in_specs=[
            pl.BlockSpec((8, LANES), lambda i: (0, 0)),
            line,
            pl.BlockSpec((rows, LANES), lambda i: (i, 0)),
            pl.BlockSpec((groups, rows, LANES), lambda i: (0, i, 0)),
            pl.BlockSpec((1, d), lambda i: (0, 0)),
            pl.BlockSpec((2 * LANES, BLOCK * LANES), lambda i: (0, 0)),
        ],
        out_specs=[line, line],
        out_shape=[jax.ShapeDtypeStruct((tokens, d), jnp.bfloat16)] * 2,
        name="final_fast",
    )(top, hidden, rstd, block_max, gain, wide)


def fits_fused(queries, keys, out_weight, residual):
    sizes = {a: lax.axis_size(a) for a in ("dp", "seq", "tp")}
    return (
        sizes["tp"] == 2
        and sizes["seq"] == 4
        and sizes["dp"] % 2 == 0
        and keys.shape[1] == HEAD_SIZE
        and out_weight.shape[1] % (64 * LANES) == 0
        and out_weight.shape[0] == queries.shape[1]
        and out_weight.shape[0] % LANES == 0
        and residual.shape[0] * 2 == queries.shape[0]
        and residual.shape[0] % 64 == 0
    )


def local(queries, keys, values, out_weight, residual, norm_gain):
    if not fits_fused(queries, keys, out_weight, residual):
        return general(queries, keys, values, out_weight, residual, norm_gain)
    gain = norm_gain.astype(jnp.float32).reshape(1, -1)
    hidden, rstd, top, block_max = fused(queries, keys, values, out_weight, residual, gain)
    return tuple(final_fast(top, hidden, rstd, block_max, gain))


def solution(mesh):
    in_specs = (
        P(("dp", "seq"), "tp"),
        P(("dp", "seq"), "tp"),
        P(("dp", "seq"), "tp"),
        P("tp", None),
        P(("dp", "seq", "tp"), None),
        P(),
    )
    out_specs = (P(("dp", "seq", "tp"), None), P(("dp", "seq", "tp"), None))
    return jax.shard_map(local, mesh=mesh, in_specs=in_specs, out_specs=out_specs, check_vma=False)
```

```python
import functools

import jax
import jax.numpy as jnp
import numpy as np
from jax import lax
from jax.experimental import pallas as pl
from jax.experimental.pallas import tpu as pltpu
from jax.sharding import PartitionSpec as P

HEAD_SIZE = 128
BLOCK = 16
softness = 0.9
scale_floor = 256.0
neg_large = -1e30
LANES = 128
AHEAD = 2
RAW = 2
ROUND_BIG = 25165824.0
Q_COEFFS = (0.8999997814, -0.5804296733, 0.1500389216, -0.0212977078, 0.0016888914)


def soft_grid(u):
    t = u - ((u + ROUND_BIG) - ROUND_BIG)
    z = t * t
    q = jnp.float32(Q_COEFFS[-1])
    for c in Q_COEFFS[-2::-1]:
        q = q * z + jnp.float32(c)
    return u - (t - t * z) * q


def spacing_of(block_max, peak):
    tensor_scale = peak / (6.0 * 448.0)
    inv = 1.0 / (6.0 * tensor_scale)
    scale = jnp.maximum(block_max * inv, scale_floor).astype(jnp.bfloat16)
    return scale, tensor_scale


def quant_rows(x, peak):
    rows, cols = x.shape
    xb = x.reshape(rows // BLOCK, BLOCK, cols)
    block_max = jnp.max(jnp.abs(xb), axis=1, keepdims=True)
    scale, tensor_scale = spacing_of(block_max, peak)
    spacing = scale.astype(jnp.float32) * tensor_scale
    payload = soft_grid(xb * (1.0 / spacing)).astype(jnp.bfloat16).astype(jnp.float32)
    return (payload * spacing).reshape(rows, cols)


def quant_kernel(peak_ref, w_ref, out_ref, *, unroll):
    peak = peak_ref[0, 0]
    rows = w_ref.shape[0]

    def step(i, carry):
        sl = pl.ds(pl.multiple_of(i * BLOCK, BLOCK), BLOCK)
        out_ref[sl, :] = quant_rows(w_ref[sl, :].astype(jnp.float32), peak).astype(jnp.bfloat16)
        return carry

    lax.fori_loop(0, rows // BLOCK, step, 0, unroll=unroll)


def quant_weight(w, peak, width, first, cols):
    rows = w.shape[0]
    skip = first // width
    return pl.pallas_call(
        functools.partial(quant_kernel, unroll=4),
        grid=(cols // width,),
        in_specs=[
            pl.BlockSpec(memory_space=pltpu.SMEM),
            pl.BlockSpec((rows, width), lambda i: (0, i + skip)),
        ],
        out_specs=pl.BlockSpec((rows, width), lambda i: (0, i)),
        out_shape=jax.ShapeDtypeStruct((rows, cols), jnp.bfloat16),
        cost_estimate=pl.CostEstimate(
            flops=40 * rows * cols, bytes_accessed=4 * rows * cols, transcendentals=0
        ),
        name="quant_weight",
    )(peak, w)


def project_kernel(*refs, n_tp, n_feat, n_alias, features):
    peak_ref, act_refs = refs[0], refs[1 : 1 + n_tp]
    own_ref, peer_ref, res_ref, gain_ref, sq_in, top_in = refs[1 + n_tp : 7 + n_tp]
    refs = refs[7 + n_tp + n_alias :]
    new_ref, hid_ref, square_sum, row_top, rstd_ref, top_ref, act_q = refs
    step_id = pl.program_id(0)

    @pl.when(step_id == 0)
    def _():
        peak = peak_ref[0, 0]
        square_sum[...] = sq_in[...]
        row_top[...] = top_in[...]
        for k in range(n_tp):
            for lo in range(0, n_feat, 128):
                x = act_refs[k][lo : lo + 128, :].astype(jnp.float32)
                act_q[k, :, lo : lo + 128] = quant_rows(x, peak).T.astype(jnp.bfloat16)

    hidden = res_ref[...].astype(jnp.float32)
    for k in range(n_tp):
        w = own_ref[...] if k == 0 else peer_ref[0, k - 1]
        part = jnp.dot(act_q[k], w, preferred_element_type=jnp.float32)
        hidden = hidden + part.astype(jnp.bfloat16).astype(jnp.float32)
    new_ref[...] = hidden.astype(jnp.bfloat16)
    hid_ref[...] = hidden
    sq = square_sum[...]
    top = row_top[...]
    scaled = jnp.abs(hidden * gain_ref[...])
    for lo in range(0, hidden.shape[1], 128):
        part = hidden[:, lo : lo + 128]
        sq = sq + part * part
        top = jnp.maximum(top, scaled[:, lo : lo + 128])
    square_sum[...] = sq
    row_top[...] = top

    @pl.when(step_id == pl.num_programs(0) - 1)
    def _():
        mean_square = jnp.sum(square_sum[...], axis=1, keepdims=True) / features
        rstd = lax.rsqrt(mean_square + 1e-05)
        rstd_ref[...] = jnp.broadcast_to(rstd, rstd_ref.shape)
        top_all = jnp.max(jnp.max(row_top[...], axis=1, keepdims=True) * rstd)
        top_ref[...] = jnp.full(top_ref.shape, top_all, jnp.float32)


def project(peak, acts, w_own, w_peer, residual, gain, stats, width, skip, wide, made):
    n_tp = len(acts)
    n_feat, tokens = acts[0].shape
    d = residual.shape[1]
    steps = w_own.shape[1] // width
    column = pl.BlockSpec((tokens, width), lambda i: (0, i + skip))
    whole = pl.BlockSpec((tokens, 128), lambda i: (0, 0))
    if wide:
        peer_spec = pl.BlockSpec((1, n_tp - 1, n_feat, width), lambda i: (0, 0, 0, i))
    else:
        peer_spec = pl.BlockSpec((1, n_tp - 1, n_feat, width), lambda i: (i, 0, 0, 0))
    stat = jax.ShapeDtypeStruct((tokens, 128), jnp.float32)
    return pl.pallas_call(
        functools.partial(project_kernel, n_tp=n_tp, n_feat=n_feat, n_alias=len(made), features=d),
        grid=(steps,),
        in_specs=[pl.BlockSpec(memory_space=pltpu.SMEM)]
        + [pl.BlockSpec((n_feat, tokens), lambda i: (0, 0))] * n_tp
        + [
            pl.BlockSpec((n_feat, width), lambda i: (0, i)),
            peer_spec,
            column,
            pl.BlockSpec((1, width), lambda i: (0, i + skip)),
            whole,
            whole,
        ]
        + [pl.BlockSpec(memory_space=pl.ANY)] * len(made),
        out_specs=[column, column, whole, whole, whole, pl.BlockSpec((8, 128), lambda i: (0, 0))],
        out_shape=[
            jax.ShapeDtypeStruct((tokens, d), jnp.bfloat16),
            jax.ShapeDtypeStruct((tokens, d), jnp.float32),
            stat,
            stat,
            stat,
            jax.ShapeDtypeStruct((8, 128), jnp.float32),
        ],
        input_output_aliases={7 + n_tp + i: i for i in range(len(made))},
        scratch_shapes=[pltpu.VMEM((n_tp, tokens, n_feat), jnp.bfloat16)],
        cost_estimate=pl.CostEstimate(
            flops=2 * n_tp * n_feat * tokens * steps * width,
            bytes_accessed=2 * n_tp * n_feat * steps * width,
            transcendentals=0,
        ),
        name="project",
    )(peak, *acts, w_own, w_peer, residual, gain, *stats, *made)


def final_kernel(peak_ref, hid_ref, rstd_ref, gain_ref, out_ref, narrow, wide):
    peak = peak_ref[0, 0]
    rows, cols = hid_ref.shape
    src = lax.broadcasted_iota(jnp.int32, (128, 128), 0)
    dst = lax.broadcasted_iota(jnp.int32, (128, 128), 1)
    spread = jnp.where(src == (dst // BLOCK) * BLOCK + BLOCK - 1, 1.0, 0.0).astype(jnp.bfloat16)
    rstd = rstd_ref[...]
    tensor_scale = peak / (6.0 * 448.0)
    pieces = cols // 128
    for i in range(pieces):
        x = hid_ref[:, i * 128 : i * 128 + 128] * rstd * gain_ref[:, i * 128 : i * 128 + 128]
        m = jnp.abs(x)
        for s in (1, 2, 4, 8):
            m = jnp.maximum(m, pltpu.roll(m, s, 1))
        narrow[i * rows : (i + 1) * rows, :] = spacing_of(m, peak)[0]
    wide[...] = jnp.dot(narrow[...], spread, preferred_element_type=jnp.float32)
    for i in range(pieces):
        x = hid_ref[:, i * 128 : i * 128 + 128] * rstd * gain_ref[:, i * 128 : i * 128 + 128]
        spacing = wide[i * rows : (i + 1) * rows, :] * tensor_scale
        payload = soft_grid(x * pl.reciprocal(spacing)).astype(jnp.bfloat16).astype(jnp.float32)
        out_ref[:, i * 128 : i * 128 + 128] = (payload * spacing).astype(jnp.bfloat16)


def final_quant(peak, hidden, rstd, gain):
    tokens, d = hidden.shape
    width = 2048
    rows = min(64, tokens)
    column = pl.BlockSpec((rows, width), lambda i, j: (i, j))
    return pl.pallas_call(
        final_kernel,
        grid=(tokens // rows, d // width),
        in_specs=[
            pl.BlockSpec(memory_space=pltpu.SMEM),
            column,
            pl.BlockSpec((rows, 128), lambda i, j: (i, 0)),
            pl.BlockSpec((1, width), lambda i, j: (0, j)),
        ],
        out_specs=column,
        out_shape=jax.ShapeDtypeStruct((tokens, d), jnp.bfloat16),
        scratch_shapes=[
            pltpu.VMEM((rows * width // 128, 128), jnp.bfloat16),
            pltpu.VMEM((rows * width // 128, 128), jnp.float32),
        ],
        name="final_quant",
    )(peak, hidden, rstd, gain)


def attend(queries, keys, values, first_query):
    token_count = queries.shape[0]
    kv_heads = keys.shape[1] // HEAD_SIZE
    grouped = queries.shape[1] // HEAD_SIZE // kv_heads
    q = queries.reshape(token_count, kv_heads, grouped, HEAD_SIZE)
    k = keys.reshape(-1, kv_heads, HEAD_SIZE)
    v = values.reshape(-1, kv_heads, HEAD_SIZE)
    scores = jnp.einsum("tkgd,skd->kgts", q, k, preferred_element_type=jnp.float32)
    scores = scores * HEAD_SIZE ** (-0.5)
    query_pos = first_query + lax.broadcasted_iota(jnp.int32, (token_count, 1), 0)
    key_pos = lax.broadcasted_iota(jnp.int32, (1, k.shape[0]), 1)
    allowed = query_pos >= key_pos
    masked = jnp.where(allowed, scores, neg_large)
    top = jnp.max(masked, axis=3, keepdims=True)
    weights = jnp.where(allowed, jnp.exp(masked - top), 0.0)
    total = jnp.sum(weights, axis=3)
    summed = jnp.einsum(
        "kgts,skd->kgtd", weights.astype(jnp.bfloat16), v, preferred_element_type=jnp.float32
    )
    attended = (summed / total[..., None]).astype(jnp.bfloat16)
    return attended.transpose(0, 1, 3, 2).reshape(-1, token_count)


def general(queries, keys, values, out_weight, residual, norm_gain):
    token_count = queries.shape[0]
    n_tp = lax.axis_size("tp")
    tp_rank = lax.axis_index("tp")
    slabs = lax.axis_size("dp") * lax.axis_size("seq")
    d = out_weight.shape[1]
    width = d // slabs
    kv = lax.all_gather(jnp.stack((keys, values)), "seq", axis=1, tiled=True)

    weight_top = jnp.max(jnp.abs(out_weight)).astype(jnp.float32)
    weight_peak = lax.pmax(weight_top, "tp").reshape(1, 1)
    slab_id = lax.axis_index("dp") * lax.axis_size("seq") + lax.axis_index("seq")
    direct = 128
    gather_w = width - direct
    gathered = slabs * gather_w
    slab = lax.dynamic_slice_in_dim(out_weight, slab_id * gather_w, gather_w, axis=1)
    slab_q = quant_weight(slab, weight_peak, gather_w, 0, gather_w)
    shifts = [[(i, (i + k) % n_tp) for i in range(n_tp)] for k in range(1, n_tp)]
    from_peers = jnp.stack([lax.ppermute(slab_q, "tp", ring) for ring in shifts])
    w_peer = lax.all_gather(from_peers, ("dp", "seq"), axis=0)
    near_own = quant_weight(out_weight, weight_peak, 512, gathered, d - gathered)
    near_peer = jnp.stack([lax.ppermute(near_own, "tp", ring) for ring in shifts])[None]
    w_own = quant_weight(out_weight, weight_peak, gather_w, 0, gathered)

    act_t = attend(queries, kv[0], kv[1], lax.axis_index("seq") * token_count)
    act_top = jnp.max(jnp.abs(act_t)).astype(jnp.float32)
    share = token_count // n_tp
    pieces = []
    for k in range(n_tp):
        whose = lax.rem(tp_rank + k, n_tp)
        piece = lax.dynamic_slice_in_dim(act_t, whose * share, share, axis=1)
        pieces.append(piece if k == 0 else lax.ppermute(piece, "tp", shifts[k - 1]))
    act_peak = lax.pmax(act_top, ("seq", "tp")).reshape(1, 1)

    gain = norm_gain.astype(jnp.float32).reshape(1, d)
    stats = (jnp.zeros((share, 128), jnp.float32),) * 2
    near = project(
        act_peak, pieces, near_own, near_peer, residual, gain, stats, 512, gathered // 512, True, ()
    )
    new_residual, hidden, _, _, rstd, top = project(
        act_peak, pieces, w_own, w_peer, residual, gain, near[2:4], gather_w, 0, False, near[:2]
    )
    norm_peak = lax.pmax(top[0, 0], ("seq", "tp")).reshape(1, 1)
    next_input = final_quant(norm_peak, hidden, rstd, gain)
    return (new_residual, next_input)


def quant_tile(src, dst, inv, tensor_scale):
    rows = src.shape[0]
    step = 128 if rows % 128 == 0 else BLOCK
    for lo in range(0, rows, step):
        x = src[lo : lo + step, :].astype(jnp.float32).reshape(step // BLOCK, BLOCK, LANES)
        block_max = jnp.max(jnp.abs(x), axis=1, keepdims=True)
        scale = jnp.maximum(block_max * inv, scale_floor).astype(jnp.bfloat16)
        spacing = scale.astype(jnp.float32) * tensor_scale
        payload = soft_grid(x * (1.0 / spacing)).astype(jnp.bfloat16).astype(jnp.float32)
        dst[lo : lo + step, :] = (payload * spacing).reshape(step, LANES).astype(jnp.bfloat16)


def scales_of(top):
    tensor_scale = top / (6.0 * 448.0)
    return 1.0 / (6.0 * tensor_scale), tensor_scale


def block_maxima(parts):
    lane = lax.broadcasted_iota(jnp.int32, parts[0].shape, 1)
    s = 1
    while s < BLOCK:
        if len(parts) == 1:
            m = parts[0]
            turned = jnp.where(lane // s % 2 == 1, pltpu.roll(m, s, 1), pltpu.roll(m, LANES - s, 1))
            parts = [jnp.maximum(m, turned)]
        else:
            parts = [
                jnp.where(
                    lane // s % 2 == 1,
                    jnp.maximum(b, pltpu.roll(b, s, 1)),
                    jnp.maximum(a, pltpu.roll(a, LANES - s, 1)),
                )
                for a, b in zip(parts[::2], parts[1::2])
            ]
        s *= 2
    return parts[0]


def two_parts(x):
    high = x.astype(jnp.bfloat16)
    low = (x - high.astype(jnp.float32)).astype(jnp.bfloat16)
    return jnp.concatenate([high, low], axis=1)


def spread_matrix():
    src = np.arange(2 * LANES)[:, None] % LANES
    dst = np.arange(BLOCK * LANES)[None, :]
    wide = src == dst % LANES // BLOCK * BLOCK + dst // LANES
    return jnp.asarray(wide, jnp.bfloat16)


def fused_kernel(
    q_hbm, k_hbm, v_hbm, w_hbm, res_hbm, gain_ref, wide_ref,
    hid_hbm, rstd_ref, top_ref, bm_ref,
    q_buf, kv_buf, raw_own, raw_peer, w_own, w_peer, res_buf, hid_buf,
    act_full, act_peer, act_q, square_sum, peaks,
    score_a, score_b, top_a, top_b, weights, total, acc, parts_a, parts_b, gain_f,
    local_sem, load_sem, recv_sem, x_sem, y_sem, z_sem,
    kv_send, kv_recv, peak_send, peak_recv, act_sem,
    own_send, own_recv, peer_send, peer_recv, out_sem,
    *, features,
):
    tokens = k_hbm.shape[0]
    heads = q_hbm.shape[1] // HEAD_SIZE
    share = res_hbm.shape[0]
    n_feat = heads * HEAD_SIZE
    tiles = raw_own.shape[0]
    group = tiles // 4
    pairs = tiles // 2
    group_pairs = group // 2
    direct = group // 4
    relays = group - direct
    dp, seq, tp = lax.axis_index("dp"), lax.axis_index("seq"), lax.axis_index("tp")
    core, y = seq % 2, seq // 2
    zz = dp % 2
    x_dev = {"dp": dp, "seq": seq, "tp": 1 - tp}
    y_dev = {"dp": dp, "seq": (1 - y) * 2 + core, "tp": tp}
    z_dev = {"dp": dp + 1 - 2 * zz, "seq": seq, "tp": tp}
    s_dev = {"dp": dp, "seq": y * 2 + 1 - core, "tp": tp}

    def remote(src, dst, send, recv, dev):
        return pltpu.make_async_remote_copy(
            src_ref=src, dst_ref=dst, send_sem=send, recv_sem=recv,
            device_id=dev, device_id_type=pl.DeviceIdType.MESH,
        )

    g_mine, g_y = y + 2 * zz, (1 - y) + 2 * zz
    g_z, g_d = y + 2 * (1 - zz), (1 - y) + 2 * (1 - zz)
    x_count = group + direct
    y_count = group + relays // 2

    col0 = core * tiles

    def tile_of(j, raw):
        return raw_peer.at[j] if raw else w_peer.at[col0 + j]

    def x_send(i):
        j = g_mine * group + i if i < group else g_d * group + relays + i - group
        src = raw_own.at[j] if i < RAW else w_own.at[col0 + j]
        return remote(src, tile_of(j, i < RAW), x_sem.at[i], recv_sem.at[j], x_dev)

    def y_send(i, j, raw=False):
        return remote(tile_of(j, raw), tile_of(j, raw), y_sem.at[i], recv_sem.at[j], y_dev)

    def z_send(i, j, raw=False):
        return remote(tile_of(j, raw), tile_of(j, raw), z_sem.at[i], recv_sem.at[j], z_dev)

    def wait_tile(j):
        remote(raw_peer.at[j], raw_peer.at[j], x_sem.at[0], recv_sem.at[j], x_dev).wait_recv()

    def forward(i):
        j = g_mine * group + i
        wait_tile(j)
        y_send(i, j, i < RAW).start()
        z_send(i, j, i < RAW).start()
        if i + AHEAD < x_count:
            x_send(i + AHEAD).start()

    def relay(t):
        if t % 2 == 0:
            j = g_z * group + t
            wait_tile(j)
            y_send(group + t // 2, j, t < RAW).start()
        else:
            j = g_y * group + t
            wait_tile(j)
            z_send(group + t // 2, j, t < RAW).start()

    def load(j):
        cols = pl.ds(pl.multiple_of((col0 + j) * LANES, LANES), LANES)
        return pltpu.make_async_copy(w_hbm.at[:, cols], raw_own.at[j], load_sem.at[j])

    k_load = pltpu.make_async_copy(k_hbm, kv_buf.at[seq, 0], local_sem.at[0])
    v_load = pltpu.make_async_copy(v_hbm, kv_buf.at[seq, 1], local_sem.at[1])
    res_load = pltpu.make_async_copy(res_hbm, res_buf, local_sem.at[2])
    q_loads = [
        pltpu.make_async_copy(
            q_hbm.at[:, h * HEAD_SIZE : (h + 1) * HEAD_SIZE], q_buf.at[h], local_sem.at[3 + h]
        )
        for h in range(heads)
    ]

    def load_order(n):
        return lax.rem(g_mine * group + n, tiles)

    def start_load(n, c):
        load(load_order(n)).start()
        return c

    k_load.start()
    v_load.start()
    lax.fori_loop(0, tiles, start_load, 0)
    for c in q_loads:
        c.start()
    res_load.start()

    barrier = pltpu.get_barrier_semaphore()
    team = []
    for ds in range(4):
        for dt in range(2):
            if ds or dt:
                team.append((ds, dt))
    for ds, dt in team:
        dev = {"dp": dp, "seq": lax.rem(seq + ds, 4), "tp": lax.rem(tp + dt, 2)}
        pl.semaphore_signal(barrier, inc=1, device_id=dev, device_id_type=pl.DeviceIdType.MESH)
    pl.semaphore_signal(barrier, inc=1, device_id=z_dev, device_id_type=pl.DeviceIdType.MESH)
    pl.semaphore_wait(barrier, len(team) + 1)

    k_load.wait()
    v_load.wait()
    other = y * 2 + 1 - core
    far = (1 - y) * 2 + core
    far_other = (1 - y) * 2 + 1 - core
    kv_y = remote(kv_buf.at[seq], kv_buf.at[seq], kv_send.at[0], kv_recv.at[seq], y_dev)
    kv_s = remote(kv_buf.at[seq], kv_buf.at[seq], kv_send.at[1], kv_recv.at[seq], s_dev)
    kv_f = remote(kv_buf.at[far], kv_buf.at[far], kv_send.at[2], kv_recv.at[far], s_dev)
    kv_y.start()
    kv_s.start()

    def wait_load(n, c):
        load(load_order(n)).wait()
        return c

    wait_load(0, 0)
    x_send(0).start()
    lax.fori_loop(1, tiles, wait_load, 0)

    def peak_exchange(kind, value, members):
        me = seq * 2 + tp
        peaks[kind, me] = value
        sends = []
        for ds, dt in members:
            ps = ds(seq) if callable(ds) else lax.rem(seq + ds, 4)
            pt = lax.rem(tp + dt, 2)
            dev = {"dp": dp, "seq": ps, "tp": pt}
            n = len(sends)
            out = remote(
                peaks.at[kind, me], peaks.at[kind, me], peak_send.at[kind, n],
                peak_recv.at[kind, me], dev,
            )
            out.start()
            sends.append((out, ps * 2 + pt))

        def finish():
            top = value
            for out, them in sends:
                remote(
                    peaks.at[kind, them], peaks.at[kind, them], peak_send.at[kind, 0],
                    peak_recv.at[kind, them], x_dev,
                ).wait_recv()
                top = jnp.maximum(top, peaks[kind, them])
            return top

        return finish, [out for out, _ in sends]

    def tile_top(j, m):
        high, low = m
        for t in range(4):
            x = raw_own[4 * j + t].reshape(-1, 8 * BLOCK, LANES)
            high = jnp.maximum(high, jnp.max(x, axis=0))
            low = jnp.minimum(low, jnp.min(x, axis=0))
        return high, low

    zero = jnp.zeros((8 * BLOCK, LANES), jnp.bfloat16)
    w_high, w_low = lax.fori_loop(0, tiles // 4, tile_top, (zero, zero))
    w_top = jnp.maximum(w_high.astype(jnp.float32), -w_low.astype(jnp.float32))
    w_top = jnp.full((8, LANES), jnp.max(w_top), jnp.float32)

    def sib(s):
        return (s // 2) * 2 + 1 - s % 2

    finish_w, w_sends = peak_exchange(0, w_top, [(sib, 0), (0, 1), (sib, 1)])

    for i in range(1, RAW):
        x_send(i).start()
    w_inv, w_scale = scales_of(finish_w()[0:1, :])

    def own_copy(p):
        sl = pl.ds(col0 + 2 * p, 2)
        return remote(w_own.at[sl], w_own.at[sl], own_send.at[p], own_recv.at[p], s_dev)

    def own_pair(p):
        for t in range(2):
            quant_tile(raw_own.at[2 * p + t], w_own.at[col0 + 2 * p + t], w_inv, w_scale)
        own_copy(p).start()

    def own_range(first, count):
        def body(n, c):
            own_pair(first + n)
            return c

        lax.fori_loop(0, count, body, 0)

    half = group_pairs
    own_range(g_mine * half + 1, 1)
    forward(0)
    own_range(g_mine * half + 2, half - 2)
    remote(kv_buf.at[far], kv_buf.at[far], kv_send.at[0], kv_recv.at[far], y_dev).wait_recv()
    kv_f.start()

    for c in q_loads:
        c.wait()
    for slot in (other, far_other):
        remote(kv_buf.at[slot], kv_buf.at[slot], kv_send.at[0], kv_recv.at[slot], s_dev).wait_recv()

    rate = HEAD_SIZE ** (-0.5) * 1.4426950408889634

    def lanes_of(x):
        return [x[:, lo : lo + LANES] for lo in range(0, tokens, LANES)]

    def scores(first, h0, b, diagonal, out, top):
        for u in range(2):
            q = q_buf[h0 + u, pl.ds(first, share), :]
            s = lax.dot_general(
                q, kv_buf[b, 0], (((1,), (1,)), ((), ())), preferred_element_type=jnp.float32
            )
            if diagonal:
                row = lax.broadcasted_iota(jnp.int32, (share, tokens), 0) + first
                col = lax.broadcasted_iota(jnp.int32, (share, tokens), 1)
                s = jnp.where(row >= col, s, neg_large)
            rows = slice(u * share, (u + 1) * share)
            out[b, rows, :] = s
            top[rows, :] = functools.reduce(jnp.maximum, lanes_of(s), top[rows, :])

    def weigh(b, source, top):
        for lo in range(0, tokens, 32):
            rows = slice(lo, lo + 32)
            shift = top[rows, :]
            p = [jnp.exp2(x * rate - shift) for x in lanes_of(source[b, rows, :])]
            total[rows, :] += functools.reduce(jnp.add, p)
            weights[rows, :] = jnp.concatenate(p, axis=1).astype(jnp.bfloat16)
        acc[...] += jnp.dot(weights[...], kv_buf[b, 1], preferred_element_type=jnp.float32)

    def attend(now, later):
        def block(b, diagonal):
            if later:
                scores(later[0], later[1], b, diagonal, later[2], later[3])
            if now:
                weigh(b, now[2], now[3])

        def body(b, c):
            block(b, False)
            return c

        if later:
            later[3][...] = jnp.full_like(later[3], neg_large)
        if now:
            total[...] = jnp.zeros_like(total)
            acc[...] = jnp.zeros_like(acc)
        lax.fori_loop(0, seq, body, 0)
        block(seq, True)
        if later:
            top = jnp.max(later[3][...], axis=1, keepdims=True) * rate
            later[3][...] = jnp.broadcast_to(top, later[3].shape)
        m = jnp.zeros((1, LANES), jnp.float32)
        if now:
            out = (acc[...] / jnp.sum(total[...], axis=1, keepdims=True)).astype(jnp.bfloat16)
            for u in range(2):
                act_full[now[1] + u, pl.ds(now[0], share), :] = out[u * share : (u + 1) * share]
            m = jnp.max(jnp.abs(out.astype(jnp.float32)), axis=0, keepdims=True)
        return m

    theirs = pl.multiple_of((1 - tp) * share, share)
    mine = pl.multiple_of(tp * share, share)
    act_copy = remote(
        act_full.at[:, pl.ds(theirs, share), :], act_peer, act_sem.at[0], act_sem.at[1], x_dev
    )
    jobs = [(theirs, 0), (theirs, 2), (mine, 0), (mine, 2)]
    jobs = [j + ((score_a, top_a) if n % 2 == 0 else (score_b, top_b)) for n, j in enumerate(jobs)]
    forward(1)
    attend(None, jobs[0])
    forward(2)
    a_top = attend(jobs[0], jobs[1])
    relay(0)
    relay(1)
    a_top = jnp.maximum(a_top, attend(jobs[1], jobs[2]))
    act_copy.start()
    a_top = jnp.maximum(a_top, attend(jobs[2], jobs[3]))
    a_top = jnp.maximum(a_top, attend(jobs[3], None))
    a_top = jnp.full((8, LANES), jnp.max(a_top), jnp.float32)
    finish_a, a_sends = peak_exchange(1, a_top, team)
    forward(3)
    own_range(g_d * half + half - 1, 1)
    own_range(g_mine * half, 1)
    forward(4)
    own_range(g_y * half, half)
    relay(2)
    own_range(g_z * half, half)
    relay(3)
    forward(5)
    own_range(g_d * half, half - 1)
    square_sum[...] = jnp.zeros_like(square_sum)

    def local_pair(p):
        late = p // (3 * group_pairs)
        sel = lax.rem(p, 3)
        fy = late + (1 - late) * (sel % 2)
        fz = late + (1 - late) * (sel // 2)
        g = lax.rem(y + fy, 2) + 2 * lax.rem(zz + fz, 2)
        i = (1 - late) * (p // 3) + late * (p - 3 * group_pairs)
        return g * group_pairs + i, late, sel, i

    def peer_copy(lp):
        sl = pl.ds(col0 + 2 * lp, 2)
        return remote(w_peer.at[sl], w_peer.at[sl], peer_send.at[lp], peer_recv.at[lp], s_dev)

    def take_raw(p):
        lp = local_pair(p)[0]
        if p == 3 * group_pairs:
            wait_tile(2 * lp)
            wait_tile(2 * lp + 1)
        elif p:
            wait_tile(2 * lp + p - 1)
        for t in range(2):
            quant_tile(raw_peer.at[2 * lp + t], w_peer.at[col0 + 2 * lp + t], w_inv, w_scale)
        peer_copy(lp).start()

    for p in (0, 1):
        take_raw(p)
    forward(6)
    relay(4)
    for p in (2, 3 * group_pairs):
        take_raw(p)

    a_inv, a_scale = scales_of(finish_a()[0:1, :])
    act_copy.wait_recv()
    def act_tile(t, lo, n):
        if t < heads:
            return act_full[t, pl.ds(mine + lo, n), :].astype(jnp.float32)
        return act_peer[t - heads, lo : lo + n, :].astype(jnp.float32)

    rates, spacings = [], []
    for lo in range(0, share, 16):
        m = block_maxima([jnp.abs(act_tile(t, lo, 16)) for t in range(2 * heads)])
        scale = jnp.maximum(m * a_inv, scale_floor).astype(jnp.bfloat16)
        spacing = scale.astype(jnp.float32) * a_scale
        rates.append(two_parts(1.0 / spacing))
        spacings.append(two_parts(spacing))
    rates = jnp.concatenate(rates, axis=0)
    spacings = jnp.concatenate(spacings, axis=0)
    for t in range(0, 2 * heads, 2):
        cols = wide_ref[:, t * LANES : (t + 2) * LANES]
        rate = jnp.dot(rates, cols, preferred_element_type=jnp.float32)
        spacing = jnp.dot(spacings, cols, preferred_element_type=jnp.float32)
        for lo in range(0, share, 32):
            x = jnp.concatenate([act_tile(t, lo, 32), act_tile(t + 1, lo, 32)], axis=1)
            payload = soft_grid(x * rate[lo : lo + 32]).astype(jnp.bfloat16).astype(jnp.float32)
            first = t % heads * LANES
            act_q[t // heads, lo : lo + 32, first : first + 2 * LANES] = (
                payload * spacing[lo : lo + 32]
            ).astype(jnp.bfloat16)

    def out_copy(n):
        cols = pl.ds(pl.multiple_of(2 * n * LANES, 2 * LANES), 2 * LANES)
        return pltpu.make_async_copy(hid_buf.at[:, cols], hid_hbm.at[:, cols], out_sem.at[n])

    lane = lax.broadcasted_iota(jnp.int32, (32, LANES), 1)

    def finish(p, parts):
        lp, _, _, i = local_pair(p)
        pair_ids = (lp, lp + pairs)
        cols = [pl.ds(pl.multiple_of(2 * n * LANES, 2 * LANES), 2 * LANES) for n in pair_ids]
        gains = [
            jnp.concatenate([gain_f[pl.ds(2 * n, 1), :], gain_f[pl.ds(2 * n + 1, 1), :]], axis=1)
            for n in pair_ids
        ]
        mask = lane // 4 % 4 == i
        turns = [LANES - s + 2 * s * ((4 * i // s) % 2) for s in (4, 8)]
        for lo in range(0, share, 32):
            rows = slice(lo, lo + 32)
            maxima = []
            squares = square_sum[rows, :]
            for u in range(2):
                p0 = parts[2 * u, rows, :].astype(jnp.bfloat16).astype(jnp.float32)
                p1 = parts[2 * u + 1, rows, :].astype(jnp.bfloat16).astype(jnp.float32)
                h = res_buf[rows, cols[u]].astype(jnp.float32) + (p0 + p1)
                hid_buf[rows, cols[u]] = h
                s = jnp.abs(h * gains[u])
                h = h * h
                squares = squares + (h[:, :LANES] + h[:, LANES:])
                maxima += [s[:, :LANES], s[:, LANES:]]
            square_sum[rows, :] = squares
            for s in (1, 2):
                maxima = [
                    jnp.where(
                        lane // s % 2 == 1,
                        jnp.maximum(b, pltpu.roll(b, s, 1)),
                        jnp.maximum(a, pltpu.roll(a, LANES - s, 1)),
                    )
                    for a, b in zip(maxima[::2], maxima[1::2])
                ]
            m = maxima[0]
            for turn in turns:
                m = jnp.maximum(m, pltpu.roll(m, turn, 1))
            g = lp // group_pairs
            bm_ref[g, rows, :] = jnp.where(mask, m, bm_ref[g, rows, :])
        for n in pair_ids:
            out_copy(n).start()

    def product(k, w, n):
        w = jnp.concatenate([w[2 * n], w[2 * n + 1]], axis=1)
        return jnp.dot(act_q[k], w, preferred_element_type=jnp.float32)

    def multiply(p, parts):
        lp = local_pair(p)[0]
        for u, n in enumerate((lp, lp + pairs)):
            parts[2 * u] = product(0, w_own, n)
            parts[2 * u + 1] = product(1, w_peer, n)

    other0 = (1 - core) * tiles

    def take(p):
        lp, late, sel, i = local_pair(p)

        @pl.when((1 - late) * sel * (i // (group_pairs - 1)) + late > 0)
        def _():
            wait_tile(2 * lp)
            wait_tile(2 * lp + 1)

        @pl.when((1 - late) * sel * (1 - i // (group_pairs - 1)) > 0)
        def _():
            wait_tile(2 * lp + sel - 1)

        peer_copy(lp).start()

    res_load.wait()
    gain_f[...] = gain_ref[...].astype(jnp.float32)
    forward(7)
    relay(5)

    def step(p, parts, before):
        @pl.when((p > 1) * (p < pairs - 1) * (p + 1 != 3 * group_pairs))
        def _():
            take(p + 1)

        lp = local_pair(p)[0]
        sl = pl.ds(other0 + 2 * lp, 2)
        remote(w_own.at[sl], w_own.at[sl], own_send.at[0], own_recv.at[lp], s_dev).wait_recv()
        remote(w_peer.at[sl], w_peer.at[sl], peer_send.at[0], peer_recv.at[lp], s_dev).wait_recv()
        multiply(p, parts)
        if before is not None:
            finish(p - 1, before)

    step(0, parts_a, None)

    def two_steps(r, c):
        p = 2 * r + 1

        step(p, parts_b, parts_a)

        step(p + 1, parts_a, parts_b)
        return c

    lax.fori_loop(0, pairs // 2 - 1, two_steps, 0)
    step(pairs - 1, parts_b, parts_a)
    finish(pairs - 1, parts_b)

    mean_square = jnp.sum(square_sum[...], axis=1, keepdims=True) / features
    rstd = lax.rsqrt(mean_square + 1e-05)
    rstd_ref[...] = jnp.broadcast_to(rstd, rstd_ref.shape)
    n_top = jnp.max(jnp.max(bm_ref[...], axis=0) * rstd)
    finish_n, n_sends = peak_exchange(2, jnp.full((8, LANES), n_top, jnp.float32), team)

    kv_y.wait_send()
    kv_s.wait_send()
    kv_f.wait_send()
    act_copy.wait_send()
    for c in w_sends + a_sends:
        c.wait_send()

    def drain(n, c):
        own_copy(n).wait_send()
        peer_copy(n).wait_send()
        out_copy(n).wait()
        out_copy(n + pairs).wait()
        return c

    lax.fori_loop(0, pairs, drain, 0)

    def drain_x(i, c):
        remote(raw_own.at[0], raw_peer.at[0], x_sem.at[i], recv_sem.at[0], x_dev).wait_send()
        return c

    lax.fori_loop(0, x_count, drain_x, 0)

    def drain_yz(i, c):
        y_send(i, 0).wait_send()
        z_send(i, 0).wait_send()
        return c

    lax.fori_loop(0, y_count, drain_yz, 0)
    top_ref[...] = finish_n()
    for c in n_sends:
        c.wait_send()


def fused(queries, keys, values, out_weight, residual, gain, wide):
    tokens, n_feat = queries.shape
    share, d = residual.shape
    heads = n_feat // HEAD_SIZE
    tiles = d // LANES // 2
    pairs = tiles // 2
    group = tiles // 4
    any_spec = pl.BlockSpec(memory_space=pl.ANY)
    vmem = pl.BlockSpec(memory_space=pltpu.VMEM)
    dma = pltpu.SemaphoreType.DMA
    bf16, f32 = jnp.bfloat16, jnp.float32
    rows = out_weight.shape[0]
    return pl.pallas_call(
        functools.partial(fused_kernel, features=d),
        in_specs=[any_spec] * 5 + [vmem] * 2,
        out_specs=[any_spec, vmem, vmem, vmem],
        out_shape=[
            jax.ShapeDtypeStruct((share, d), f32),
            jax.ShapeDtypeStruct((share, LANES), f32),
            jax.ShapeDtypeStruct((8, LANES), f32),
            jax.ShapeDtypeStruct((d // (BLOCK * LANES), share, LANES), f32),
        ],
        scratch_shapes=[
            pltpu.VMEM((heads, tokens, HEAD_SIZE), bf16),
            pltpu.VMEM((4, 2, tokens, HEAD_SIZE), bf16),
            pltpu.VMEM((tiles, rows, LANES), bf16),
            pltpu.VMEM((tiles, rows, LANES), bf16),
            pltpu.VMEM((2 * tiles, rows, LANES), bf16),
            pltpu.VMEM((2 * tiles, rows, LANES), bf16),
            pltpu.VMEM((share, d), bf16),
            pltpu.VMEM((share, d), f32),
            pltpu.VMEM((heads, tokens, HEAD_SIZE), bf16),
            pltpu.VMEM((heads, share, HEAD_SIZE), bf16),
            pltpu.VMEM((2, share, n_feat), bf16),
            pltpu.VMEM((share, LANES), f32),
            pltpu.VMEM((3, 8, 8, LANES), f32),
            pltpu.VMEM((4, tokens, tokens), f32),
            pltpu.VMEM((4, tokens, tokens), f32),
            pltpu.VMEM((tokens, LANES), f32),
            pltpu.VMEM((tokens, LANES), f32),
            pltpu.VMEM((tokens, tokens), bf16),
            pltpu.VMEM((tokens, LANES), f32),
            pltpu.VMEM((tokens, HEAD_SIZE), f32),
            pltpu.VMEM((4, share, 2 * LANES), f32),
            pltpu.VMEM((4, share, 2 * LANES), f32),
            pltpu.VMEM((d // LANES, LANES), f32),
            dma((3 + heads,)),
            dma((tiles,)),
            dma((tiles,)),
            dma((group + group // 4,)),
            dma((group + 3 * group // 8,)),
            dma((group + 3 * group // 8,)),
            dma((3,)),
            dma((4,)),
            dma((3, 7)),
            dma((3, 8)),
            dma((2,)),
            dma((pairs,)),
            dma((pairs,)),
            dma((pairs,)),
            dma((pairs,)),
            dma((2 * pairs,)),
        ],
        compiler_params=pltpu.CompilerParams(
            collective_id=0, has_side_effects=True, vmem_limit_bytes=60 * 1024 * 1024
        ),
        name="fused",
    )(queries, keys, values, out_weight, residual, gain, wide)


def final_fast_kernel(top_ref, hid_ref, rstd_ref, bm_ref, gain_ref, wide_ref, new_ref, out_ref):
    rows, d = hid_ref.shape
    groups = bm_ref.shape[0]
    inv, tensor_scale = scales_of(top_ref[0:1, :])
    gains = gain_ref[...].astype(jnp.float32)
    rstd = rstd_ref[...]
    rates, spacings = [], []
    for g in range(groups):
        scale = jnp.maximum(bm_ref[g] * rstd * inv, scale_floor).astype(jnp.bfloat16)
        spacing = scale.astype(jnp.float32) * tensor_scale
        rates.append(two_parts(rstd / spacing))
        spacings.append(two_parts(spacing))
    rates = jnp.concatenate(rates, axis=0)
    spacings = jnp.concatenate(spacings, axis=0)
    width = 2 * LANES
    for v in range(BLOCK // 2):
        wide = wide_ref[:, v * width : (v + 1) * width]
        rate = jnp.dot(rates, wide, preferred_element_type=jnp.float32)
        spacing = jnp.dot(spacings, wide, preferred_element_type=jnp.float32)
        for g in range(groups):
            pair = g * (BLOCK // 4) + v // 2 + v % 2 * (d // (2 * width))
            lo = pair * width
            h = hid_ref[:, lo : lo + width]
            new_ref[:, lo : lo + width] = h.astype(jnp.bfloat16)
            gain = jnp.concatenate([gains[2 * pair + t : 2 * pair + t + 1] for t in (0, 1)], axis=1)
            u = (h * gain) * rate[g * rows : (g + 1) * rows]
            payload = soft_grid(u).astype(jnp.bfloat16).astype(jnp.float32)
            out_ref[:, lo : lo + width] = (payload * spacing[g * rows : (g + 1) * rows]).astype(
                jnp.bfloat16
            )


def final_fast(top, hidden, rstd, block_max, gain, wide):
    tokens, d = hidden.shape
    rows = 64
    groups = block_max.shape[0]
    line = pl.BlockSpec((rows, d), lambda i: (i, 0))
    return pl.pallas_call(
        final_fast_kernel,
        grid=(tokens // rows,),
        in_specs=[
            pl.BlockSpec((8, LANES), lambda i: (0, 0)),
            line,
            pl.BlockSpec((rows, LANES), lambda i: (i, 0)),
            pl.BlockSpec((groups, rows, LANES), lambda i: (0, i, 0)),
            pl.BlockSpec((d // LANES, LANES), lambda i: (0, 0)),
            pl.BlockSpec((2 * LANES, BLOCK * LANES), lambda i: (0, 0)),
        ],
        out_specs=[line, line],
        out_shape=[jax.ShapeDtypeStruct((tokens, d), jnp.bfloat16)] * 2,
        name="final_fast",
    )(top, hidden, rstd, block_max, gain, wide)


def fits_fused(queries, keys, out_weight, residual):
    sizes = {a: lax.axis_size(a) for a in ("dp", "seq", "tp")}
    return (
        sizes["tp"] == 2
        and sizes["seq"] == 4
        and sizes["dp"] % 2 == 0
        and keys.shape[1] == HEAD_SIZE
        and queries.shape[1] == 4 * HEAD_SIZE
        and out_weight.shape[1] % (64 * LANES) == 0
        and out_weight.shape[0] == queries.shape[1]
        and out_weight.shape[0] % LANES == 0
        and residual.shape[0] * 2 == queries.shape[0]
        and residual.shape[0] % 64 == 0
    )


def local(queries, keys, values, out_weight, residual, norm_gain):
    if not fits_fused(queries, keys, out_weight, residual):
        return general(queries, keys, values, out_weight, residual, norm_gain)
    gain = norm_gain.reshape(-1, LANES)
    wide = spread_matrix()
    hidden, rstd, top, block_max = fused(queries, keys, values, out_weight, residual, gain, wide)
    return tuple(final_fast(top, hidden, rstd, block_max, gain, wide))


def solution(mesh):
    in_specs = (
        P(("dp", "seq"), "tp"),
        P(("dp", "seq"), "tp"),
        P(("dp", "seq"), "tp"),
        P("tp", None),
        P(("dp", "seq", "tp"), None),
        P(),
    )
    out_specs = (P(("dp", "seq", "tp"), None), P(("dp", "seq", "tp"), None))
    return jax.shard_map(local, mesh=mesh, in_specs=in_specs, out_specs=out_specs, check_vma=False)
```

```python
import functools

import jax
import jax.numpy as jnp
import numpy as np
from jax import lax
from jax.experimental import pallas as pl
from jax.experimental.pallas import tpu as pltpu
from jax.sharding import PartitionSpec as P

HEAD_SIZE = 128
BLOCK = 16
softness = 0.9
scale_floor = 256.0
neg_large = -1e30
LANES = 128
AHEAD = 2
AHEAD_PAIRS = 2
RAW = 2
ROUND_BIG = 25165824.0
Q_COEFFS = (0.8999997814, -0.5804296733, 0.1500389216, -0.0212977078, 0.0016888914)


def soft_grid(u):
    t = u - ((u + ROUND_BIG) - ROUND_BIG)
    z = t * t
    q = jnp.float32(Q_COEFFS[-1])
    for c in Q_COEFFS[-2::-1]:
        q = q * z + jnp.float32(c)
    return u - (t - t * z) * q


def spacing_of(block_max, peak):
    tensor_scale = peak / (6.0 * 448.0)
    inv = 1.0 / (6.0 * tensor_scale)
    scale = jnp.maximum(block_max * inv, scale_floor).astype(jnp.bfloat16)
    return scale, tensor_scale


def quant_rows(x, peak):
    rows, cols = x.shape
    xb = x.reshape(rows // BLOCK, BLOCK, cols)
    block_max = jnp.max(jnp.abs(xb), axis=1, keepdims=True)
    scale, tensor_scale = spacing_of(block_max, peak)
    spacing = scale.astype(jnp.float32) * tensor_scale
    payload = soft_grid(xb * (1.0 / spacing)).astype(jnp.bfloat16).astype(jnp.float32)
    return (payload * spacing).reshape(rows, cols)


def quant_kernel(peak_ref, w_ref, out_ref, *, unroll):
    peak = peak_ref[0, 0]
    rows = w_ref.shape[0]

    def step(i, carry):
        sl = pl.ds(pl.multiple_of(i * BLOCK, BLOCK), BLOCK)
        out_ref[sl, :] = quant_rows(w_ref[sl, :].astype(jnp.float32), peak).astype(jnp.bfloat16)
        return carry

    lax.fori_loop(0, rows // BLOCK, step, 0, unroll=unroll)


def quant_weight(w, peak, width, first, cols):
    rows = w.shape[0]
    skip = first // width
    return pl.pallas_call(
        functools.partial(quant_kernel, unroll=4),
        grid=(cols // width,),
        in_specs=[
            pl.BlockSpec(memory_space=pltpu.SMEM),
            pl.BlockSpec((rows, width), lambda i: (0, i + skip)),
        ],
        out_specs=pl.BlockSpec((rows, width), lambda i: (0, i)),
        out_shape=jax.ShapeDtypeStruct((rows, cols), jnp.bfloat16),
        cost_estimate=pl.CostEstimate(
            flops=40 * rows * cols, bytes_accessed=4 * rows * cols, transcendentals=0
        ),
        name="quant_weight",
    )(peak, w)


def project_kernel(*refs, n_tp, n_feat, n_alias, features):
    peak_ref, act_refs = refs[0], refs[1 : 1 + n_tp]
    own_ref, peer_ref, res_ref, gain_ref, sq_in, top_in = refs[1 + n_tp : 7 + n_tp]
    refs = refs[7 + n_tp + n_alias :]
    new_ref, hid_ref, square_sum, row_top, rstd_ref, top_ref, act_q = refs
    step_id = pl.program_id(0)

    @pl.when(step_id == 0)
    def _():
        peak = peak_ref[0, 0]
        square_sum[...] = sq_in[...]
        row_top[...] = top_in[...]
        for k in range(n_tp):
            for lo in range(0, n_feat, 128):
                x = act_refs[k][lo : lo + 128, :].astype(jnp.float32)
                act_q[k, :, lo : lo + 128] = quant_rows(x, peak).T.astype(jnp.bfloat16)

    hidden = res_ref[...].astype(jnp.float32)
    for k in range(n_tp):
        w = own_ref[...] if k == 0 else peer_ref[0, k - 1]
        part = jnp.dot(act_q[k], w, preferred_element_type=jnp.float32)
        hidden = hidden + part.astype(jnp.bfloat16).astype(jnp.float32)
    new_ref[...] = hidden.astype(jnp.bfloat16)
    hid_ref[...] = hidden
    sq = square_sum[...]
    top = row_top[...]
    scaled = jnp.abs(hidden * gain_ref[...])
    for lo in range(0, hidden.shape[1], 128):
        part = hidden[:, lo : lo + 128]
        sq = sq + part * part
        top = jnp.maximum(top, scaled[:, lo : lo + 128])
    square_sum[...] = sq
    row_top[...] = top

    @pl.when(step_id == pl.num_programs(0) - 1)
    def _():
        mean_square = jnp.sum(square_sum[...], axis=1, keepdims=True) / features
        rstd = lax.rsqrt(mean_square + 1e-05)
        rstd_ref[...] = jnp.broadcast_to(rstd, rstd_ref.shape)
        top_all = jnp.max(jnp.max(row_top[...], axis=1, keepdims=True) * rstd)
        top_ref[...] = jnp.full(top_ref.shape, top_all, jnp.float32)


def project(peak, acts, w_own, w_peer, residual, gain, stats, width, skip, wide, made):
    n_tp = len(acts)
    n_feat, tokens = acts[0].shape
    d = residual.shape[1]
    steps = w_own.shape[1] // width
    column = pl.BlockSpec((tokens, width), lambda i: (0, i + skip))
    whole = pl.BlockSpec((tokens, 128), lambda i: (0, 0))
    if wide:
        peer_spec = pl.BlockSpec((1, n_tp - 1, n_feat, width), lambda i: (0, 0, 0, i))
    else:
        peer_spec = pl.BlockSpec((1, n_tp - 1, n_feat, width), lambda i: (i, 0, 0, 0))
    stat = jax.ShapeDtypeStruct((tokens, 128), jnp.float32)
    return pl.pallas_call(
        functools.partial(project_kernel, n_tp=n_tp, n_feat=n_feat, n_alias=len(made), features=d),
        grid=(steps,),
        in_specs=[pl.BlockSpec(memory_space=pltpu.SMEM)]
        + [pl.BlockSpec((n_feat, tokens), lambda i: (0, 0))] * n_tp
        + [
            pl.BlockSpec((n_feat, width), lambda i: (0, i)),
            peer_spec,
            column,
            pl.BlockSpec((1, width), lambda i: (0, i + skip)),
            whole,
            whole,
        ]
        + [pl.BlockSpec(memory_space=pl.ANY)] * len(made),
        out_specs=[column, column, whole, whole, whole, pl.BlockSpec((8, 128), lambda i: (0, 0))],
        out_shape=[
            jax.ShapeDtypeStruct((tokens, d), jnp.bfloat16),
            jax.ShapeDtypeStruct((tokens, d), jnp.float32),
            stat,
            stat,
            stat,
            jax.ShapeDtypeStruct((8, 128), jnp.float32),
        ],
        input_output_aliases={7 + n_tp + i: i for i in range(len(made))},
        scratch_shapes=[pltpu.VMEM((n_tp, tokens, n_feat), jnp.bfloat16)],
        cost_estimate=pl.CostEstimate(
            flops=2 * n_tp * n_feat * tokens * steps * width,
            bytes_accessed=2 * n_tp * n_feat * steps * width,
            transcendentals=0,
        ),
        name="project",
    )(peak, *acts, w_own, w_peer, residual, gain, *stats, *made)


def final_kernel(peak_ref, hid_ref, rstd_ref, gain_ref, out_ref, narrow, wide):
    peak = peak_ref[0, 0]
    rows, cols = hid_ref.shape
    src = lax.broadcasted_iota(jnp.int32, (128, 128), 0)
    dst = lax.broadcasted_iota(jnp.int32, (128, 128), 1)
    spread = jnp.where(src == (dst // BLOCK) * BLOCK + BLOCK - 1, 1.0, 0.0).astype(jnp.bfloat16)
    rstd = rstd_ref[...]
    tensor_scale = peak / (6.0 * 448.0)
    pieces = cols // 128
    for i in range(pieces):
        x = hid_ref[:, i * 128 : i * 128 + 128] * rstd * gain_ref[:, i * 128 : i * 128 + 128]
        m = jnp.abs(x)
        for s in (1, 2, 4, 8):
            m = jnp.maximum(m, pltpu.roll(m, s, 1))
        narrow[i * rows : (i + 1) * rows, :] = spacing_of(m, peak)[0]
    wide[...] = jnp.dot(narrow[...], spread, preferred_element_type=jnp.float32)
    for i in range(pieces):
        x = hid_ref[:, i * 128 : i * 128 + 128] * rstd * gain_ref[:, i * 128 : i * 128 + 128]
        spacing = wide[i * rows : (i + 1) * rows, :] * tensor_scale
        payload = soft_grid(x * pl.reciprocal(spacing)).astype(jnp.bfloat16).astype(jnp.float32)
        out_ref[:, i * 128 : i * 128 + 128] = (payload * spacing).astype(jnp.bfloat16)


def final_quant(peak, hidden, rstd, gain):
    tokens, d = hidden.shape
    width = 2048
    rows = min(64, tokens)
    column = pl.BlockSpec((rows, width), lambda i, j: (i, j))
    return pl.pallas_call(
        final_kernel,
        grid=(tokens // rows, d // width),
        in_specs=[
            pl.BlockSpec(memory_space=pltpu.SMEM),
            column,
            pl.BlockSpec((rows, 128), lambda i, j: (i, 0)),
            pl.BlockSpec((1, width), lambda i, j: (0, j)),
        ],
        out_specs=column,
        out_shape=jax.ShapeDtypeStruct((tokens, d), jnp.bfloat16),
        scratch_shapes=[
            pltpu.VMEM((rows * width // 128, 128), jnp.bfloat16),
            pltpu.VMEM((rows * width // 128, 128), jnp.float32),
        ],
        name="final_quant",
    )(peak, hidden, rstd, gain)


def attend(queries, keys, values, first_query):
    token_count = queries.shape[0]
    kv_heads = keys.shape[1] // HEAD_SIZE
    grouped = queries.shape[1] // HEAD_SIZE // kv_heads
    q = queries.reshape(token_count, kv_heads, grouped, HEAD_SIZE)
    k = keys.reshape(-1, kv_heads, HEAD_SIZE)
    v = values.reshape(-1, kv_heads, HEAD_SIZE)
    scores = jnp.einsum("tkgd,skd->kgts", q, k, preferred_element_type=jnp.float32)
    scores = scores * HEAD_SIZE ** (-0.5)
    query_pos = first_query + lax.broadcasted_iota(jnp.int32, (token_count, 1), 0)
    key_pos = lax.broadcasted_iota(jnp.int32, (1, k.shape[0]), 1)
    allowed = query_pos >= key_pos
    masked = jnp.where(allowed, scores, neg_large)
    top = jnp.max(masked, axis=3, keepdims=True)
    weights = jnp.where(allowed, jnp.exp(masked - top), 0.0)
    total = jnp.sum(weights, axis=3)
    summed = jnp.einsum(
        "kgts,skd->kgtd", weights.astype(jnp.bfloat16), v, preferred_element_type=jnp.float32
    )
    attended = (summed / total[..., None]).astype(jnp.bfloat16)
    return attended.transpose(0, 1, 3, 2).reshape(-1, token_count)


def general(queries, keys, values, out_weight, residual, norm_gain):
    token_count = queries.shape[0]
    n_tp = lax.axis_size("tp")
    tp_rank = lax.axis_index("tp")
    slabs = lax.axis_size("dp") * lax.axis_size("seq")
    d = out_weight.shape[1]
    width = d // slabs
    kv = lax.all_gather(jnp.stack((keys, values)), "seq", axis=1, tiled=True)

    weight_top = jnp.max(jnp.abs(out_weight)).astype(jnp.float32)
    weight_peak = lax.pmax(weight_top, "tp").reshape(1, 1)
    slab_id = lax.axis_index("dp") * lax.axis_size("seq") + lax.axis_index("seq")
    direct = 128
    gather_w = width - direct
    gathered = slabs * gather_w
    slab = lax.dynamic_slice_in_dim(out_weight, slab_id * gather_w, gather_w, axis=1)
    slab_q = quant_weight(slab, weight_peak, gather_w, 0, gather_w)
    shifts = [[(i, (i + k) % n_tp) for i in range(n_tp)] for k in range(1, n_tp)]
    from_peers = jnp.stack([lax.ppermute(slab_q, "tp", ring) for ring in shifts])
    w_peer = lax.all_gather(from_peers, ("dp", "seq"), axis=0)
    near_own = quant_weight(out_weight, weight_peak, 512, gathered, d - gathered)
    near_peer = jnp.stack([lax.ppermute(near_own, "tp", ring) for ring in shifts])[None]
    w_own = quant_weight(out_weight, weight_peak, gather_w, 0, gathered)

    act_t = attend(queries, kv[0], kv[1], lax.axis_index("seq") * token_count)
    act_top = jnp.max(jnp.abs(act_t)).astype(jnp.float32)
    share = token_count // n_tp
    pieces = []
    for k in range(n_tp):
        whose = lax.rem(tp_rank + k, n_tp)
        piece = lax.dynamic_slice_in_dim(act_t, whose * share, share, axis=1)
        pieces.append(piece if k == 0 else lax.ppermute(piece, "tp", shifts[k - 1]))
    act_peak = lax.pmax(act_top, ("seq", "tp")).reshape(1, 1)

    gain = norm_gain.astype(jnp.float32).reshape(1, d)
    stats = (jnp.zeros((share, 128), jnp.float32),) * 2
    near = project(
        act_peak, pieces, near_own, near_peer, residual, gain, stats, 512, gathered // 512, True, ()
    )
    new_residual, hidden, _, _, rstd, top = project(
        act_peak, pieces, w_own, w_peer, residual, gain, near[2:4], gather_w, 0, False, near[:2]
    )
    norm_peak = lax.pmax(top[0, 0], ("seq", "tp")).reshape(1, 1)
    next_input = final_quant(norm_peak, hidden, rstd, gain)
    return (new_residual, next_input)


def row_maxima(parts):
    row = lax.broadcasted_iota(jnp.int32, parts[0].shape, 0)
    half = len(parts) // 2
    low = row < 4
    parts = [
        jnp.maximum(jnp.where(low, a, b), pltpu.roll(jnp.where(low, b, a), 4, 0))
        for a, b in zip(parts[:half], parts[half:])
    ]
    for s in (2, 1):
        half //= 2
        even = row // s % 2 == 0
        parts = [
            jnp.maximum(
                jnp.where(even, a, b),
                jnp.where(even, pltpu.roll(a, 8 - s, 0), pltpu.roll(b, s, 0)),
            )
            for a, b in zip(parts[:half], parts[half:])
        ]
    return parts[0]


def quant_tile(src, dst, inv, tensor_scale, rate_buf, space_buf):
    rows = src.shape[0]
    for lo in range(0, rows, 8 * BLOCK):
        parts = []
        for b in range(lo, lo + 8 * BLOCK, BLOCK):
            x = jnp.abs(src[b : b + BLOCK, :].astype(jnp.float32))
            parts.append(jnp.maximum(x[:8], x[8:]))
        scale = jnp.maximum(row_maxima(parts) * inv, scale_floor).astype(jnp.bfloat16)
        spacing = scale.astype(jnp.float32) * tensor_scale
        rate_buf[lo // BLOCK : lo // BLOCK + 8, :] = 1.0 / spacing
        space_buf[lo // BLOCK : lo // BLOCK + 8, :] = spacing
    for b in range(0, rows, BLOCK):
        n = b // BLOCK
        x = src[b : b + BLOCK, :].astype(jnp.float32)
        payload = soft_grid(x * rate_buf[n : n + 1, :]).astype(jnp.bfloat16).astype(jnp.float32)
        dst[b : b + BLOCK, :] = (payload * space_buf[n : n + 1, :]).astype(jnp.bfloat16)


def scales_of(top):
    tensor_scale = top / (6.0 * 448.0)
    return 1.0 / (6.0 * tensor_scale), tensor_scale


def block_maxima(parts):
    lane = lax.broadcasted_iota(jnp.int32, parts[0].shape, 1)
    s = 1
    while s < BLOCK:
        if len(parts) == 1:
            m = parts[0]
            turned = jnp.where(lane // s % 2 == 1, pltpu.roll(m, s, 1), pltpu.roll(m, LANES - s, 1))
            parts = [jnp.maximum(m, turned)]
        else:
            parts = [
                jnp.where(
                    lane // s % 2 == 1,
                    jnp.maximum(b, pltpu.roll(b, s, 1)),
                    jnp.maximum(a, pltpu.roll(a, LANES - s, 1)),
                )
                for a, b in zip(parts[::2], parts[1::2])
            ]
        s *= 2
    return parts[0]


def two_parts(x):
    high = x.astype(jnp.bfloat16)
    low = (x - high.astype(jnp.float32)).astype(jnp.bfloat16)
    return jnp.concatenate([high, low], axis=1)


def spread_matrix():
    src = np.arange(2 * LANES)[:, None] % LANES
    dst = np.arange(BLOCK * LANES)[None, :]
    wide = src == dst % LANES // BLOCK * BLOCK + dst // LANES
    return jnp.asarray(wide, jnp.bfloat16)


def fused_kernel(
    q_hbm, k_hbm, v_hbm, w_hbm, res_hbm, gain_ref, wide_ref,
    hid_hbm, rstd_ref, top_ref, bm_ref,
    q_buf, kv_buf, raw_own, raw_peer, w_own, w_peer, res_buf, hid_buf,
    act_full, act_peer, act_q, square_sum, peaks, rate_buf, space_buf,
    score_a, score_b, top_a, top_b, weights, total, acc, parts_a, parts_b, gain_f,
    local_sem, load_sem, recv_sem, x_sem, y_sem, z_sem,
    kv_send, kv_recv, peak_send, peak_recv, act_sem,
    own_send, own_recv, peer_send, peer_recv, out_sem,
    *, features,
):
    tokens = k_hbm.shape[0]
    heads = q_hbm.shape[1] // HEAD_SIZE
    share = res_hbm.shape[0]
    n_feat = heads * HEAD_SIZE
    tiles = raw_own.shape[0]
    group = tiles // 4
    pairs = tiles // 2
    group_pairs = group // 2
    direct = group // 4
    relays = group - direct
    dp, seq, tp = lax.axis_index("dp"), lax.axis_index("seq"), lax.axis_index("tp")
    core, y = seq % 2, seq // 2
    zz = dp % 2
    x_dev = {"dp": dp, "seq": seq, "tp": 1 - tp}
    y_dev = {"dp": dp, "seq": (1 - y) * 2 + core, "tp": tp}
    z_dev = {"dp": dp + 1 - 2 * zz, "seq": seq, "tp": tp}
    s_dev = {"dp": dp, "seq": y * 2 + 1 - core, "tp": tp}

    def remote(src, dst, send, recv, dev):
        return pltpu.make_async_remote_copy(
            src_ref=src, dst_ref=dst, send_sem=send, recv_sem=recv,
            device_id=dev, device_id_type=pl.DeviceIdType.MESH,
        )

    g_mine, g_y = y + 2 * zz, (1 - y) + 2 * zz
    g_z, g_d = y + 2 * (1 - zz), (1 - y) + 2 * (1 - zz)
    x_count = group + direct
    y_count = group + relays // 2

    col0 = core * tiles

    def tile_of(j, raw):
        return raw_peer.at[j] if raw else w_peer.at[col0 + j]

    def x_send(i):
        j = g_mine * group + i if i < group else g_d * group + relays + i - group
        src = raw_own.at[j] if i < RAW else w_own.at[col0 + j]
        return remote(src, tile_of(j, i < RAW), x_sem.at[i], recv_sem.at[j], x_dev)

    def y_send(i, j, raw=False):
        return remote(tile_of(j, raw), tile_of(j, raw), y_sem.at[i], recv_sem.at[j], y_dev)

    def z_send(i, j, raw=False):
        return remote(tile_of(j, raw), tile_of(j, raw), z_sem.at[i], recv_sem.at[j], z_dev)

    def wait_tile(j):
        remote(raw_peer.at[j], raw_peer.at[j], x_sem.at[0], recv_sem.at[j], x_dev).wait_recv()

    def forward(i):
        j = g_mine * group + i
        wait_tile(j)
        y_send(i, j, i < RAW).start()
        z_send(i, j, i < RAW).start()
        if i + AHEAD < x_count:
            x_send(i + AHEAD).start()

    def relay(t):
        if t % 2 == 0:
            j = g_z * group + t
            wait_tile(j)
            y_send(group + t // 2, j, t < RAW).start()
        else:
            j = g_y * group + t
            wait_tile(j)
            z_send(group + t // 2, j, t < RAW).start()

    def load(j):
        cols = pl.ds(pl.multiple_of((col0 + j) * LANES, LANES), LANES)
        return pltpu.make_async_copy(w_hbm.at[:, cols], raw_own.at[j], load_sem.at[j])

    k_load = pltpu.make_async_copy(k_hbm, kv_buf.at[seq, 0], local_sem.at[0])
    v_load = pltpu.make_async_copy(v_hbm, kv_buf.at[seq, 1], local_sem.at[1])
    res_load = pltpu.make_async_copy(res_hbm, res_buf, local_sem.at[2])
    q_loads = [
        pltpu.make_async_copy(
            q_hbm.at[:, h * HEAD_SIZE : (h + 1) * HEAD_SIZE], q_buf.at[h], local_sem.at[3 + h]
        )
        for h in range(heads)
    ]

    def load_order(n):
        return lax.rem(g_mine * group + n, tiles)

    def start_load(n, c):
        load(load_order(n)).start()
        return c

    k_load.start()
    v_load.start()
    lax.fori_loop(0, tiles, start_load, 0)
    for c in q_loads:
        c.start()
    res_load.start()

    barrier = pltpu.get_barrier_semaphore()
    team = []
    for ds in range(4):
        for dt in range(2):
            if ds or dt:
                team.append((ds, dt))
    for ds, dt in team:
        dev = {"dp": dp, "seq": lax.rem(seq + ds, 4), "tp": lax.rem(tp + dt, 2)}
        pl.semaphore_signal(barrier, inc=1, device_id=dev, device_id_type=pl.DeviceIdType.MESH)
    pl.semaphore_signal(barrier, inc=1, device_id=z_dev, device_id_type=pl.DeviceIdType.MESH)
    pl.semaphore_wait(barrier, len(team) + 1)

    k_load.wait()
    v_load.wait()
    other = y * 2 + 1 - core
    far = (1 - y) * 2 + core
    far_other = (1 - y) * 2 + 1 - core
    def kv_copy(part, n, slot, dev):
        ref = kv_buf.at[slot, part]
        return remote(ref, ref, kv_send.at[part, n], kv_recv.at[part, slot], dev)

    kv_sends = [kv_copy(part, n, seq, dev) for part in range(2) for n, dev in ((0, y_dev), (1, s_dev))]
    for c in kv_sends:
        c.start()
    kv_onward = [kv_copy(part, 2, far, s_dev) for part in range(2)]

    def kv_pass(part):
        kv_copy(part, 0, far, y_dev).wait_recv()
        kv_onward[part].start()

    def kv_rest(part):
        for slot in (other, far_other):
            kv_copy(part, 1, slot, s_dev).wait_recv()

    load(load_order(0)).wait()
    x_send(0).start()

    def peak_exchange(kind, value, members):
        me = seq * 2 + tp
        peaks[kind, me] = value
        sends = []
        for ds, dt in members:
            ps = ds(seq) if callable(ds) else lax.rem(seq + ds, 4)
            pt = lax.rem(tp + dt, 2)
            dev = {"dp": dp, "seq": ps, "tp": pt}
            n = len(sends)
            out = remote(
                peaks.at[kind, me], peaks.at[kind, me], peak_send.at[kind, n],
                peak_recv.at[kind, me], dev,
            )
            out.start()
            sends.append((out, ps * 2 + pt))

        def finish():
            top = value
            for out, them in sends:
                remote(
                    peaks.at[kind, them], peaks.at[kind, them], peak_send.at[kind, 0],
                    peak_recv.at[kind, them], x_dev,
                ).wait_recv()
                top = jnp.maximum(top, peaks[kind, them])
            return top

        return finish, [out for out, _ in sends]

    def tile_top(j, m):
        high, low = m
        for t in range(4):
            n = load_order(4 * j + t)
            if t:
                load(n).wait()
            else:
                @pl.when(j > 0)
                def _():
                    load(n).wait()

        for t in range(4):
            x = raw_own[load_order(4 * j + t)].reshape(-1, 8 * BLOCK, LANES)
            high = jnp.maximum(high, jnp.max(x, axis=0))
            low = jnp.minimum(low, jnp.min(x, axis=0))
        return high, low

    zero = jnp.zeros((8 * BLOCK, LANES), jnp.bfloat16)
    w_high, w_low = lax.fori_loop(0, tiles // 4, tile_top, (zero, zero))
    w_top = jnp.maximum(w_high.astype(jnp.float32), -w_low.astype(jnp.float32))
    w_top = jnp.full((8, LANES), jnp.max(w_top), jnp.float32)

    def sib(s):
        return (s // 2) * 2 + 1 - s % 2

    finish_w, w_sends = peak_exchange(0, w_top, [(sib, 0), (0, 1), (sib, 1)])

    for i in range(1, RAW):
        x_send(i).start()
    w_inv, w_scale = scales_of(finish_w()[0:1, :])

    def own_copy(p):
        sl = pl.ds(col0 + 2 * p, 2)
        return remote(w_own.at[sl], w_own.at[sl], own_send.at[p], own_recv.at[p], s_dev)

    def own_pair(p):
        for t in range(2):
            quant_tile(raw_own.at[2 * p + t], w_own.at[col0 + 2 * p + t], w_inv, w_scale, rate_buf.at[t], space_buf.at[t])
        own_copy(p).start()

    def own_range(first, count):
        def body(n, c):
            own_pair(first + n)
            return c

        lax.fori_loop(0, count, body, 0)

    half = group_pairs
    kv_pass(0)
    own_range(g_mine * half + 1, 1)
    forward(0)
    own_range(g_mine * half + 2, half - 2)
    forward(1)
    kv_pass(1)

    for c in q_loads:
        c.wait()
    kv_rest(0)

    rate = HEAD_SIZE ** (-0.5) * 1.4426950408889634

    def lanes_of(x):
        return [x[:, lo : lo + LANES] for lo in range(0, tokens, LANES)]

    def scores(first, h0, b, diagonal, out, top):
        for u in range(2):
            q = q_buf[h0 + u, pl.ds(first, share), :]
            s = lax.dot_general(
                q, kv_buf[b, 0], (((1,), (1,)), ((), ())), preferred_element_type=jnp.float32
            )
            if diagonal:
                row = lax.broadcasted_iota(jnp.int32, (share, tokens), 0) + first
                col = lax.broadcasted_iota(jnp.int32, (share, tokens), 1)
                s = jnp.where(row >= col, s, neg_large)
            rows = slice(u * share, (u + 1) * share)
            out[b, rows, :] = s
            top[rows, :] = functools.reduce(jnp.maximum, lanes_of(s), top[rows, :])

    def weigh(b, source, top):
        for lo in range(0, tokens, 32):
            rows = slice(lo, lo + 32)
            shift = top[rows, :]
            p = [jnp.exp2(x * rate - shift) for x in lanes_of(source[b, rows, :])]
            total[rows, :] += functools.reduce(jnp.add, p)
            weights[rows, :] = jnp.concatenate(p, axis=1).astype(jnp.bfloat16)
        acc[...] += jnp.dot(weights[...], kv_buf[b, 1], preferred_element_type=jnp.float32)

    def attend(now, later):
        def block(b, diagonal):
            if later:
                scores(later[0], later[1], b, diagonal, later[2], later[3])
            if now:
                weigh(b, now[2], now[3])

        def body(b, c):
            block(b, False)
            return c

        if later:
            later[3][...] = jnp.full_like(later[3], neg_large)
        if now:
            total[...] = jnp.zeros_like(total)
            acc[...] = jnp.zeros_like(acc)
        lax.fori_loop(0, seq, body, 0)
        block(seq, True)
        if later:
            top = jnp.max(later[3][...], axis=1, keepdims=True) * rate
            later[3][...] = jnp.broadcast_to(top, later[3].shape)
        m = jnp.zeros((1, LANES), jnp.float32)
        if now:
            out = (acc[...] / jnp.sum(total[...], axis=1, keepdims=True)).astype(jnp.bfloat16)
            for u in range(2):
                act_full[now[1] + u, pl.ds(now[0], share), :] = out[u * share : (u + 1) * share]
            m = jnp.max(jnp.abs(out.astype(jnp.float32)), axis=0, keepdims=True)
        return m

    theirs = pl.multiple_of((1 - tp) * share, share)
    mine = pl.multiple_of(tp * share, share)
    act_copy = remote(
        act_full.at[:, pl.ds(theirs, share), :], act_peer, act_sem.at[0], act_sem.at[1], x_dev
    )
    jobs = [(theirs, 0), (theirs, 2), (mine, 0), (mine, 2)]
    jobs = [j + ((score_a, top_a) if n % 2 == 0 else (score_b, top_b)) for n, j in enumerate(jobs)]
    attend(None, jobs[0])
    kv_rest(1)
    a_top = attend(jobs[0], jobs[1])
    forward(2)
    a_top = jnp.maximum(a_top, attend(jobs[1], jobs[2]))
    act_copy.start()
    relay(0)
    relay(1)
    a_top = jnp.maximum(a_top, attend(jobs[2], jobs[3]))
    a_top = jnp.maximum(a_top, attend(jobs[3], None))
    a_top = jnp.full((8, LANES), jnp.max(a_top), jnp.float32)
    finish_a, a_sends = peak_exchange(1, a_top, team)
    forward(3)
    own_range(g_d * half + half - 1, 1)
    own_range(g_mine * half, 1)
    forward(4)
    own_range(g_y * half, half)
    relay(2)
    own_range(g_z * half, half)
    relay(3)
    own_range(g_d * half, half - 1)
    square_sum[...] = jnp.zeros_like(square_sum)

    def local_pair(p):
        late = p // (3 * group_pairs)
        sel = lax.rem(p, 3)
        fy = late + (1 - late) * (sel % 2)
        fz = late + (1 - late) * (sel // 2)
        g = lax.rem(y + fy, 2) + 2 * lax.rem(zz + fz, 2)
        i = (1 - late) * (p // 3) + late * (p - 3 * group_pairs)
        return g * group_pairs + i, late, sel, i

    def peer_copy(lp):
        sl = pl.ds(col0 + 2 * lp, 2)
        return remote(w_peer.at[sl], w_peer.at[sl], peer_send.at[lp], peer_recv.at[lp], s_dev)

    def take_raw(p):
        lp = local_pair(p)[0]
        if p == 3 * group_pairs:
            wait_tile(2 * lp)
            wait_tile(2 * lp + 1)
        elif p:
            wait_tile(2 * lp + p - 1)
        for t in range(2):
            quant_tile(raw_peer.at[2 * lp + t], w_peer.at[col0 + 2 * lp + t], w_inv, w_scale, rate_buf.at[t], space_buf.at[t])
        peer_copy(lp).start()

    for p in (0, 1):
        take_raw(p)
    forward(5)
    relay(4)
    for p in (2, 3 * group_pairs):
        take_raw(p)

    a_inv, a_scale = scales_of(finish_a()[0:1, :])
    act_copy.wait_recv()
    def act_tile(t, lo, n):
        if t < heads:
            return act_full[t, pl.ds(mine + lo, n), :].astype(jnp.float32)
        return act_peer[t - heads, lo : lo + n, :].astype(jnp.float32)

    rates, spacings = [], []
    for lo in range(0, share, 16):
        m = block_maxima([jnp.abs(act_tile(t, lo, 16)) for t in range(2 * heads)])
        scale = jnp.maximum(m * a_inv, scale_floor).astype(jnp.bfloat16)
        spacing = scale.astype(jnp.float32) * a_scale
        rates.append(two_parts(1.0 / spacing))
        spacings.append(two_parts(spacing))
    rates = jnp.concatenate(rates, axis=0)
    spacings = jnp.concatenate(spacings, axis=0)
    for t in range(0, 2 * heads, 2):
        cols = wide_ref[:, t * LANES : (t + 2) * LANES]
        rate = jnp.dot(rates, cols, preferred_element_type=jnp.float32)
        spacing = jnp.dot(spacings, cols, preferred_element_type=jnp.float32)
        for lo in range(0, share, 32):
            x = jnp.concatenate([act_tile(t, lo, 32), act_tile(t + 1, lo, 32)], axis=1)
            payload = soft_grid(x * rate[lo : lo + 32]).astype(jnp.bfloat16).astype(jnp.float32)
            first = t % heads * LANES
            act_q[t // heads, lo : lo + 32, first : first + 2 * LANES] = (
                payload * spacing[lo : lo + 32]
            ).astype(jnp.bfloat16)

    def out_copy(n):
        cols = pl.ds(pl.multiple_of(2 * n * LANES, 2 * LANES), 2 * LANES)
        return pltpu.make_async_copy(hid_buf.at[:, cols], hid_hbm.at[:, cols], out_sem.at[n])

    lane = lax.broadcasted_iota(jnp.int32, (32, LANES), 1)

    def finish(p, parts):
        lp, _, _, i = local_pair(p)
        pair_ids = (lp, lp + pairs)
        cols = [pl.ds(pl.multiple_of(2 * n * LANES, 2 * LANES), 2 * LANES) for n in pair_ids]
        gains = [
            jnp.concatenate([gain_f[pl.ds(2 * n, 1), :], gain_f[pl.ds(2 * n + 1, 1), :]], axis=1)
            for n in pair_ids
        ]
        mask = lane // 4 % 4 == i
        turns = [LANES - s + 2 * s * ((4 * i // s) % 2) for s in (4, 8)]
        for lo in range(0, share, 32):
            rows = slice(lo, lo + 32)
            maxima = []
            squares = square_sum[rows, :]
            for u in range(2):
                p0 = parts[2 * u, rows, :].astype(jnp.bfloat16).astype(jnp.float32)
                p1 = parts[2 * u + 1, rows, :].astype(jnp.bfloat16).astype(jnp.float32)
                h = res_buf[rows, cols[u]].astype(jnp.float32) + (p0 + p1)
                hid_buf[rows, cols[u]] = h
                s = jnp.abs(h * gains[u])
                h = h * h
                squares = squares + (h[:, :LANES] + h[:, LANES:])
                maxima += [s[:, :LANES], s[:, LANES:]]
            square_sum[rows, :] = squares
            for s in (1, 2):
                maxima = [
                    jnp.where(
                        lane // s % 2 == 1,
                        jnp.maximum(b, pltpu.roll(b, s, 1)),
                        jnp.maximum(a, pltpu.roll(a, LANES - s, 1)),
                    )
                    for a, b in zip(maxima[::2], maxima[1::2])
                ]
            m = maxima[0]
            for turn in turns:
                m = jnp.maximum(m, pltpu.roll(m, turn, 1))
            g = lp // group_pairs
            bm_ref[g, rows, :] = jnp.where(mask, m, bm_ref[g, rows, :])
        for n in pair_ids:
            out_copy(n).start()

    def product(k, w, n):
        w = jnp.concatenate([w[2 * n], w[2 * n + 1]], axis=1)
        return jnp.dot(act_q[k], w, preferred_element_type=jnp.float32)

    def multiply(p, parts):
        lp = local_pair(p)[0]
        for u, n in enumerate((lp, lp + pairs)):
            parts[2 * u] = product(0, w_own, n)
            parts[2 * u + 1] = product(1, w_peer, n)

    other0 = (1 - core) * tiles

    def take(p):
        lp, late, sel, i = local_pair(p)

        @pl.when((1 - late) * sel * (i // (group_pairs - 1)) + late > 0)
        def _():
            wait_tile(2 * lp)
            wait_tile(2 * lp + 1)

        @pl.when((1 - late) * sel * (1 - i // (group_pairs - 1)) > 0)
        def _():
            wait_tile(2 * lp + sel - 1)

        peer_copy(lp).start()

    forward(6)
    res_load.wait()
    gain_f[...] = gain_ref[...].astype(jnp.float32)

    def step(p, parts, before):
        @pl.when((p > 2 - AHEAD_PAIRS) * (p < pairs - AHEAD_PAIRS) * (p + AHEAD_PAIRS != 3 * group_pairs))
        def _():
            take(p + AHEAD_PAIRS)

        lp = local_pair(p)[0]
        sl = pl.ds(other0 + 2 * lp, 2)
        remote(w_own.at[sl], w_own.at[sl], own_send.at[0], own_recv.at[lp], s_dev).wait_recv()
        remote(w_peer.at[sl], w_peer.at[sl], peer_send.at[0], peer_recv.at[lp], s_dev).wait_recv()
        multiply(p, parts)
        if before is not None:
            finish(p - 1, before)

    step(0, parts_a, None)

    def two_steps(r, c):
        p = 2 * r + 1

        @pl.when(r == 0)
        def _():
            relay(5)

        @pl.when(r == 1)
        def _():
            forward(7)

        step(p, parts_b, parts_a)

        step(p + 1, parts_a, parts_b)
        return c

    lax.fori_loop(0, pairs // 2 - 1, two_steps, 0)
    step(pairs - 1, parts_b, parts_a)
    finish(pairs - 1, parts_b)

    mean_square = jnp.sum(square_sum[...], axis=1, keepdims=True) / features
    rstd = lax.rsqrt(mean_square + 1e-05)
    rstd_ref[...] = jnp.broadcast_to(rstd, rstd_ref.shape)
    n_top = jnp.max(jnp.max(bm_ref[...], axis=0) * rstd)
    finish_n, n_sends = peak_exchange(2, jnp.full((8, LANES), n_top, jnp.float32), team)

    for c in kv_sends + kv_onward:
        c.wait_send()
    act_copy.wait_send()
    for c in w_sends + a_sends:
        c.wait_send()

    def drain(n, c):
        own_copy(n).wait_send()
        peer_copy(n).wait_send()
        out_copy(n).wait()
        out_copy(n + pairs).wait()
        return c

    lax.fori_loop(0, pairs, drain, 0)

    def drain_x(i, c):
        remote(raw_own.at[0], raw_peer.at[0], x_sem.at[i], recv_sem.at[0], x_dev).wait_send()
        return c

    lax.fori_loop(0, x_count, drain_x, 0)

    def drain_yz(i, c):
        y_send(i, 0).wait_send()
        z_send(i, 0).wait_send()
        return c

    lax.fori_loop(0, y_count, drain_yz, 0)
    top_ref[...] = finish_n()
    for c in n_sends:
        c.wait_send()


def fused(queries, keys, values, out_weight, residual, gain, wide):
    tokens, n_feat = queries.shape
    share, d = residual.shape
    heads = n_feat // HEAD_SIZE
    tiles = d // LANES // 2
    pairs = tiles // 2
    group = tiles // 4
    any_spec = pl.BlockSpec(memory_space=pl.ANY)
    vmem = pl.BlockSpec(memory_space=pltpu.VMEM)
    dma = pltpu.SemaphoreType.DMA
    bf16, f32 = jnp.bfloat16, jnp.float32
    rows = out_weight.shape[0]
    return pl.pallas_call(
        functools.partial(fused_kernel, features=d),
        in_specs=[any_spec] * 5 + [vmem] * 2,
        out_specs=[any_spec, vmem, vmem, vmem],
        out_shape=[
            jax.ShapeDtypeStruct((share, d), f32),
            jax.ShapeDtypeStruct((share, LANES), f32),
            jax.ShapeDtypeStruct((8, LANES), f32),
            jax.ShapeDtypeStruct((d // (BLOCK * LANES), share, LANES), f32),
        ],
        scratch_shapes=[
            pltpu.VMEM((heads, tokens, HEAD_SIZE), bf16),
            pltpu.VMEM((4, 2, tokens, HEAD_SIZE), bf16),
            pltpu.VMEM((tiles, rows, LANES), bf16),
            pltpu.VMEM((tiles, rows, LANES), bf16),
            pltpu.VMEM((2 * tiles, rows, LANES), bf16),
            pltpu.VMEM((2 * tiles, rows, LANES), bf16),
            pltpu.VMEM((share, d), bf16),
            pltpu.VMEM((share, d), f32),
            pltpu.VMEM((heads, tokens, HEAD_SIZE), bf16),
            pltpu.VMEM((heads, share, HEAD_SIZE), bf16),
            pltpu.VMEM((2, share, n_feat), bf16),
            pltpu.VMEM((share, LANES), f32),
            pltpu.VMEM((3, 8, 8, LANES), f32),
            pltpu.VMEM((2, rows // BLOCK, LANES), f32),
            pltpu.VMEM((2, rows // BLOCK, LANES), f32),
            pltpu.VMEM((4, tokens, tokens), f32),
            pltpu.VMEM((4, tokens, tokens), f32),
            pltpu.VMEM((tokens, LANES), f32),
            pltpu.VMEM((tokens, LANES), f32),
            pltpu.VMEM((tokens, tokens), bf16),
            pltpu.VMEM((tokens, LANES), f32),
            pltpu.VMEM((tokens, HEAD_SIZE), f32),
            pltpu.VMEM((4, share, 2 * LANES), f32),
            pltpu.VMEM((4, share, 2 * LANES), f32),
            pltpu.VMEM((d // LANES, LANES), f32),
            dma((3 + heads,)),
            dma((tiles,)),
            dma((tiles,)),
            dma((group + group // 4,)),
            dma((group + 3 * group // 8,)),
            dma((group + 3 * group // 8,)),
            dma((2, 3)),
            dma((2, 4)),
            dma((3, 7)),
            dma((3, 8)),
            dma((2,)),
            dma((pairs,)),
            dma((pairs,)),
            dma((pairs,)),
            dma((pairs,)),
            dma((2 * pairs,)),
        ],
        compiler_params=pltpu.CompilerParams(
            collective_id=0, has_side_effects=True, vmem_limit_bytes=60 * 1024 * 1024
        ),
        name="fused",
    )(queries, keys, values, out_weight, residual, gain, wide)


def final_fast_kernel(top_ref, hid_ref, rstd_ref, bm_ref, gain_ref, wide_ref, new_ref, out_ref):
    rows, d = hid_ref.shape
    groups = bm_ref.shape[0]
    inv, tensor_scale = scales_of(top_ref[0:1, :])
    gains = gain_ref[...].astype(jnp.float32)
    rstd = rstd_ref[...]
    rates, spacings = [], []
    for g in range(groups):
        scale = jnp.maximum(bm_ref[g] * rstd * inv, scale_floor).astype(jnp.bfloat16)
        spacing = scale.astype(jnp.float32) * tensor_scale
        rates.append(two_parts(rstd / spacing))
        spacings.append(two_parts(spacing))
    rates = jnp.concatenate(rates, axis=0)
    spacings = jnp.concatenate(spacings, axis=0)
    width = 2 * LANES
    for v in range(BLOCK // 2):
        wide = wide_ref[:, v * width : (v + 1) * width]
        rate = jnp.dot(rates, wide, preferred_element_type=jnp.float32)
        spacing = jnp.dot(spacings, wide, preferred_element_type=jnp.float32)
        for g in range(groups):
            pair = g * (BLOCK // 4) + v // 2 + v % 2 * (d // (2 * width))
            lo = pair * width
            h = hid_ref[:, lo : lo + width]
            new_ref[:, lo : lo + width] = h.astype(jnp.bfloat16)
            gain = jnp.concatenate([gains[2 * pair + t : 2 * pair + t + 1] for t in (0, 1)], axis=1)
            u = (h * gain) * rate[g * rows : (g + 1) * rows]
            payload = soft_grid(u).astype(jnp.bfloat16).astype(jnp.float32)
            out_ref[:, lo : lo + width] = (payload * spacing[g * rows : (g + 1) * rows]).astype(
                jnp.bfloat16
            )


def final_fast(top, hidden, rstd, block_max, gain, wide):
    tokens, d = hidden.shape
    rows = 64
    groups = block_max.shape[0]
    line = pl.BlockSpec((rows, d), lambda i: (i, 0))
    return pl.pallas_call(
        final_fast_kernel,
        grid=(tokens // rows,),
        in_specs=[
            pl.BlockSpec((8, LANES), lambda i: (0, 0)),
            line,
            pl.BlockSpec((rows, LANES), lambda i: (i, 0)),
            pl.BlockSpec((groups, rows, LANES), lambda i: (0, i, 0)),
            pl.BlockSpec((d // LANES, LANES), lambda i: (0, 0)),
            pl.BlockSpec((2 * LANES, BLOCK * LANES), lambda i: (0, 0)),
        ],
        out_specs=[line, line],
        out_shape=[jax.ShapeDtypeStruct((tokens, d), jnp.bfloat16)] * 2,
        name="final_fast",
    )(top, hidden, rstd, block_max, gain, wide)


def fits_fused(queries, keys, out_weight, residual):
    sizes = {a: lax.axis_size(a) for a in ("dp", "seq", "tp")}
    return (
        sizes["tp"] == 2
        and sizes["seq"] == 4
        and sizes["dp"] % 2 == 0
        and keys.shape[1] == HEAD_SIZE
        and queries.shape[1] == 4 * HEAD_SIZE
        and out_weight.shape[1] % (64 * LANES) == 0
        and out_weight.shape[0] == queries.shape[1]
        and out_weight.shape[0] % LANES == 0
        and residual.shape[0] * 2 == queries.shape[0]
        and residual.shape[0] % 64 == 0
    )


def local(queries, keys, values, out_weight, residual, norm_gain):
    if not fits_fused(queries, keys, out_weight, residual):
        return general(queries, keys, values, out_weight, residual, norm_gain)
    gain = norm_gain.reshape(-1, LANES)
    wide = spread_matrix()
    hidden, rstd, top, block_max = fused(queries, keys, values, out_weight, residual, gain, wide)
    return tuple(final_fast(top, hidden, rstd, block_max, gain, wide))


def solution(mesh):
    in_specs = (
        P(("dp", "seq"), "tp"),
        P(("dp", "seq"), "tp"),
        P(("dp", "seq"), "tp"),
        P("tp", None),
        P(("dp", "seq", "tp"), None),
        P(),
    )
    out_specs = (P(("dp", "seq", "tp"), None), P(("dp", "seq", "tp"), None))
    return jax.shard_map(local, mesh=mesh, in_specs=in_specs, out_specs=out_specs, check_vma=False)
```
